256 devices in a mesh: row: 32 (over y, z), col: 8 (over x, core).
Axes of the slice: x: 4, y: 4, z: 8, core: 2. Of those that a mesh axis runs over, the one named last changes fastest.
Arguments:
- phase: float32 [512, 1024, 1024], P(None, 'row', 'col'), may hold values from -24 to 24
- pairs: int32 [512, 2], replicated, may hold values from 0 to 127, as said below
Outputs:
- solution: float32 [128, 1024, 1024], P(None, 'row', 'col')
The draws below stay inside these ranges and needn't reach their ends.
Inputs may be any that keep to these rules, and one draw needn't show every extreme that they name: `pairs`: each row holds two different dates, the earlier one first.
All inputs are finite; a program needn't handle non-finite values.
Results may differ from the reference program's by a relative error of at most 0.00018.
Values sent between devices are 32-bit elements; how exact they have to be, the bound alone decides.
A program may use at most 128 MiB of HBM per device.

```python
import jax
import jax.numpy as jnp
from jax import lax

ND = 128
M = 512
ITERS = 3
NR = 1024
NC = 1024


def draw_phase(key, part):
    key_base = jax.random.fold_in(key, 11)
    key_rough = jax.random.fold_in(key, 13)
    base = jax.random.normal(key_base, (M, NR, NC), jnp.float32)
    row_pos = jnp.arange(NR, dtype=jnp.float32) / NR
    col_pos = jnp.arange(NC, dtype=jnp.float32) / NC
    rough = jax.random.uniform(key_rough, (NR, NC), jnp.float32, 1.0, 2.0)
    scale = 3.0 ** row_pos[:, None] * 3.0 ** col_pos[None, :] * rough / 3.0
    values = base * scale * 1.5
    return jnp.clip(values, -24.0, 24.0)


def draw_pairs(key, part):
    key_first = jax.random.fold_in(key, 21)
    key_offset = jax.random.fold_in(key, 22)
    first = jax.random.randint(key_first, (M,), 0, ND)
    offset = jax.random.randint(key_offset, (M,), 1, ND)
    second = (first + offset) % ND
    return jnp.stack([jnp.minimum(first, second), jnp.maximum(first, second)], axis=1).astype(jnp.int32)


def setup_inputs(seed: int = 0) -> dict:
    key_list = jax.random.split(jax.random.key(seed), 3)
    return {
        "phase": draw_phase(jax.random.fold_in(key_list[2], 71), 0),
        "pairs": draw_pairs(jax.random.fold_in(key_list[2], 71), 0),
    }


reg_weight = 0.8

def stencil(padded):
    beside = padded[:, 2:, 1:-1] + padded[:, :-2, 1:-1] + padded[:, 1:-1, 2:] + padded[:, 1:-1, :-2]
    return 4.0 * padded[:, 1:-1, 1:-1] - beside

def laplace(field):
    return stencil(jnp.pad(field, ((0, 0), (1, 1), (1, 1))))

def design(pairs):
    dates = jnp.arange(ND, dtype=jnp.int32)
    later = (dates[None, :] == pairs[:, 1:2]).astype(jnp.float32)
    earlier = (dates[None, :] == pairs[:, 0:1]).astype(jnp.float32)
    return later - earlier

def apply_design(matrix, field):
    flat = field.reshape(field.shape[0], -1)
    result = jnp.dot(matrix, flat, precision=lax.Precision.HIGHEST, preferred_element_type=jnp.float32)
    return result.reshape((matrix.shape[0],) + field.shape[1:])

def reference(phase, pairs):
    matrix = design(pairs)
    transpose = matrix.T
    beta_norm = jnp.sqrt(jnp.sum(phase * phase))
    left_data = phase / beta_norm
    pulled = apply_design(transpose, left_data)
    alpha_norm = jnp.sqrt(jnp.sum(pulled * pulled))
    right_vec = pulled / alpha_norm
    left_reg = jnp.zeros((ND, NR, NC), jnp.float32)
    search_dir = right_vec
    solution = jnp.zeros_like(right_vec)
    phi_bar = beta_norm
    rho_bar = alpha_norm
    for step in range(ITERS):
        fwd_data = apply_design(matrix, right_vec) - alpha_norm * left_data
        fwd_reg = reg_weight * laplace(right_vec) - alpha_norm * left_reg
        beta_norm = jnp.sqrt(jnp.sum(fwd_data * fwd_data) + jnp.sum(fwd_reg * fwd_reg))
        left_data = fwd_data / beta_norm
        left_reg = fwd_reg / beta_norm
        pulled = apply_design(transpose, left_data) + reg_weight * laplace(left_reg) - beta_norm * right_vec
        alpha_norm = jnp.sqrt(jnp.sum(pulled * pulled))
        right_vec = pulled / alpha_norm
        rho_new = jnp.sqrt(rho_bar * rho_bar + beta_norm * beta_norm)
        cosine = rho_bar / rho_new
        sine_val = beta_norm / rho_new
        theta_val = sine_val * alpha_norm
        rho_bar = -cosine * alpha_norm
        phi_new = cosine * phi_bar
        phi_bar = sine_val * phi_bar
        solution = solution + phi_new / rho_new * search_dir
        search_dir = right_vec - theta_val / rho_new * search_dir
    return solution
```

```python
import jax
import jax.numpy as jnp
from jax import lax
from jax.experimental import pallas as pl
from jax.experimental.pallas import tpu as pltpu
from jax.sharding import PartitionSpec as P

ND = 128
LAM2 = 0.8 * 0.8
HALO = 5
PAD = 16
DIST_COL = 8
MESH = pl.DeviceIdType.MESH
F32 = jnp.float32
BF16 = jnp.bfloat16


def split(x):
    hi = x.astype(BF16)
    return hi, (x - hi.astype(F32)).astype(BF16)


def krylov_kernel(
    grid_rows, grid_cols, depth_rows,
    phase_ref, pairs_ref, out_ref,
    ph, z, w1, q1, w2, q2, zt, p1t, p2t, xt, nmat, acc, tot, in1, in2, in3, cmask,
    load_sem, store_sem, halo_send, halo_recv, s1s, s1r, s2s, s2r, s3s, s3r,
):
    rows, cols = ph.shape[0], ph.shape[2]
    wide = cols + 2 * DIST_COL
    row, col = lax.axis_index("row"), lax.axis_index("col")
    y_len = grid_rows // depth_rows
    row_y, row_z = row // depth_rows, lax.rem(row, depth_rows)

    first, last = PAD, PAD + cols
    total_rows = rows + 2 * HALO

    def clear_sides(e, carry):
        z[e, 0:PAD, :] = jnp.zeros((PAD, ND), F32)
        z[e, last:last + PAD, :] = jnp.zeros((PAD, ND), F32)
        return carry

    def clear_ends(e, carry):
        for base in (0, HALO + rows):
            z[base + e, first:last, :] = jnp.zeros((cols, ND), F32)
        return carry

    def load(r):
        return pltpu.make_async_copy(phase_ref.at[:, r, 0, :], ph.at[r], load_sem.at[r])

    order = [0, 1, 2, 3, 4, 5, 26, 27, 28, 29, 30, 31] + list(range(6, 26))
    for r in order:
        load(r).start()

    lax.fori_loop(0, total_rows, clear_sides, 0)
    lax.fori_loop(0, HALO, clear_ends, 0)

    around = [(-1, 0), (1, 0), (0, -1), (0, 1), (-1, -1), (-1, 1), (1, -1), (1, 1)]

    def exists(dr, dc):
        ok = jnp.bool_(True)
        if dr < 0:
            ok = row > 0
        if dr > 0:
            ok = row < grid_rows - 1
        if dc < 0:
            ok = ok & (col > 0)
        if dc > 0:
            ok = ok & (col < grid_cols - 1)
        return ok

    def col_peer(k):
        return (row, lax.rem(col + k, grid_cols))

    def y_peer(k):
        return (lax.rem(row_y + k, y_len) * depth_rows + row_z, col)

    def z_peer(k):
        return (row_y * depth_rows + lax.rem(row_z + k, depth_rows), col)

    groups = [
        (grid_cols, col, col_peer, in1, s1s, s1r),
        (y_len, row_y, y_peer, in2, s2s, s2r),
        (depth_rows, row_z, z_peer, in3, s3s, s3r),
    ]
    barrier = pltpu.get_barrier_semaphore()
    for dr, dc in around:
        @pl.when(exists(dr, dc))
        def _():
            pl.semaphore_signal(barrier, inc=1, device_id=(row + dr, col + dc), device_id_type=MESH)
    for size, _me, peer, _buf, _s, _r in groups:
        for k in range(1, size):
            pl.semaphore_signal(barrier, inc=1, device_id=peer(k), device_id_type=MESH)

    dates = lax.broadcasted_iota(jnp.int32, (ND, pairs_ref.shape[1]), 0)
    later = (dates == pairs_ref[1:2, :]).astype(F32)
    earlier = (dates == pairs_ref[0:1, :]).astype(F32)
    gt = (later - earlier).astype(BF16)
    normal = lax.dot_general(gt, gt, (((1,), (1,)), ((), ())), preferred_element_type=F32)
    eye = (
        lax.broadcasted_iota(jnp.int32, (ND, ND), 0) == lax.broadcasted_iota(jnp.int32, (ND, ND), 1)
    )
    trace = jnp.sum(jnp.where(eye, normal, 0.0), keepdims=True)
    frob = jnp.sum(normal * normal, keepdims=True)
    shift = jnp.floor(frob / trace + 20.0 * LAM2 + 0.5)
    shifted = normal - jnp.where(eye, shift, 0.0)
    n_hi = shifted.astype(BF16)
    n_lo = (shifted - n_hi.astype(F32)).astype(BF16)
    both = jnp.concatenate([n_hi, n_lo], axis=1)
    nmat[...] = jnp.concatenate([both, both], axis=0)

    side = lax.broadcasted_iota(jnp.int32, (wide, ND), 0)
    left_ok = jnp.where(col > 0, 1.0, 0.0)
    right_ok = jnp.where(col < grid_cols - 1, 1.0, 0.0)
    cmask[...] = jnp.where(
        side < DIST_COL, left_ok, jnp.where(side >= DIST_COL + cols, right_ok, 1.0)
    )
    top_ok = jnp.where(row > 0, 1.0, 0.0)
    bottom_ok = jnp.where(row < grid_rows - 1, 1.0, 0.0)
    def make_z(r):
        a_hi, a_lo = split(ph[r])
        b_hi, b_lo = split(ph[r + 1])
        hi = jnp.concatenate([a_hi, b_hi], axis=1)
        lo = jnp.concatenate([a_lo, b_lo], axis=1)
        field = jnp.dot(gt, hi, preferred_element_type=F32) + jnp.dot(gt, lo, preferred_element_type=F32)
        for i in range(2):
            part = field[:, i * cols:(i + 1) * cols]
            zt[r + i] = part
            z[HALO + r + i, first:last, :] = part.T

    def z_rows(lo, hi):
        def step(i, carry):
            r = lo + 2 * i
            load(r).wait()
            load(r + 1).wait()
            make_z(r)
            return carry
        lax.fori_loop(0, (hi - lo) // 2, step, 0)

    z_rows(0, 6)
    z_rows(26, 32)

    n_peers = sum(size - 1 for size, *_ in groups)
    n_around = jnp.int32(0)
    for dr, dc in around:
        n_around = n_around + jnp.where(exists(dr, dc), 1, 0)
    pl.semaphore_wait(barrier, n_around + n_peers)

    edge_c = {-1: first, 1: last - DIST_COL, 0: first}
    size_c = {-1: DIST_COL, 1: DIST_COL, 0: cols}
    land_c = {-1: last, 1: first - DIST_COL, 0: first}
    edge_r = {-1: HALO, 1: rows, 0: HALO}
    land_r = {-1: HALO + rows, 1: 0, 0: HALO}
    size_r = {-1: HALO, 1: HALO, 0: rows}

    def halo(i, dr, dc):
        return pltpu.make_async_remote_copy(
            src_ref=z.at[pl.ds(edge_r[dr], size_r[dr]), pl.ds(edge_c[dc], size_c[dc]), :],
            dst_ref=z.at[pl.ds(land_r[dr], size_r[dr]), pl.ds(land_c[dc], size_c[dc]), :],
            send_sem=halo_send.at[i],
            recv_sem=halo_recv.at[i],
            device_id=(row + dr, col + dc),
            device_id_type=MESH,
        )

    def send(i):
        dr, dc = around[i]
        @pl.when(exists(dr, dc))
        def _():
            halo(i, dr, dc).start()

    def arrived(i):
        dr, dc = around[i]
        @pl.when(exists(-dr, -dc))
        def _():
            halo(i, dr, dc).wait_recv()

    for i in (0, 1, 4, 5, 6, 7):
        send(i)
    z_rows(6, 26)
    for i in (2, 3):
        send(i)

    acc[...] = jnp.zeros_like(acc)
    work = pl.ds(PAD - DIST_COL, wide)
    before = pl.ds(PAD - DIST_COL - 1, wide)
    after = pl.ds(PAD - DIST_COL + 1, wide)

    def lap(buf, e):
        beside = buf[e - 1, work, :] + buf[e + 1, work, :] + buf[e, before, :] + buf[e, after, :]
        return 4.0 * buf[e, work, :] - beside

    def row_mask(e):
        return jnp.where(e < HALO, top_ok, jnp.where(e >= HALO + rows, bottom_ok, 1.0))

    def normal_times(value):
        hi, lo = split(value)
        both = jnp.dot(jnp.concatenate([hi, lo], axis=1), nmat[...], preferred_element_type=F32)
        return both[:, :ND] + both[:, ND:]

    def add_to(j, value):
        own = value[DIST_COL:DIST_COL + cols, :]
        acc[j] += jnp.sum(own.reshape(cols // 8, 8, ND), axis=0)

    def each(lo, hi, body):
        def step(e, carry):
            body(e)
            return carry
        lax.fori_loop(lo, hi, step, 0)

    def lap_rows(src, dst, lo, hi):
        def body(e):
            dst[e, work, :] = lap(src, e) * (cmask[...] * row_mask(e))
        each(lo, hi, body)

    def k_rows(src, lap_buf, dst, lo, hi, moments):
        def body(e):
            value = src[e, work, :]
            result = (normal_times(value) + LAM2 * lap(lap_buf, e)) * (cmask[...] * row_mask(e))
            dst[e, work, :] = result
            if moments is not None:
                if moments == 1:
                    add_to(0, value * value)
                add_to(moments, value * result)
                add_to(moments + 1, result * result)
        each(lo, hi, body)

    def last_rows(lo, hi):
        def body(e):
            value = q2[e, work, :]
            bent = lap(q2, e)
            add_to(5, value * normal_times(value) + LAM2 * (bent * bent))
        each(lo, hi, body)

    for i in (2, 3):
        arrived(i)
    lap_rows(z, w1, 6, 36)
    k_rows(z, w1, q1, 7, 35, 1)
    lap_rows(q1, w2, 8, 34)
    k_rows(q1, w2, q2, 9, 33, 3)
    last_rows(10, 32)

    for i in (0, 1, 4, 5, 6, 7):
        arrived(i)
    for lo, hi in ((1, 6), (36, 41)):
        lap_rows(z, w1, lo, hi)
    k_rows(z, w1, q1, 2, 5, None)
    k_rows(z, w1, q1, 5, 7, 1)
    k_rows(z, w1, q1, 35, 37, 1)
    k_rows(z, w1, q1, 37, 40, None)
    for lo, hi in ((3, 8), (34, 39)):
        lap_rows(q1, w2, lo, hi)
    k_rows(q1, w2, q2, 4, 5, None)
    k_rows(q1, w2, q2, 5, 9, 3)
    k_rows(q1, w2, q2, 33, 37, 3)
    k_rows(q1, w2, q2, 37, 38, None)
    last_rows(5, 10)
    last_rows(32, 37)

    tot[0] = jnp.concatenate([jnp.sum(acc[j], axis=0, keepdims=True) for j in range(8)], axis=0)

    def group_copy(stage, k):
        size, me, peer, buf, s_sem, r_sem = groups[stage]
        return pltpu.make_async_remote_copy(
            src_ref=tot.at[stage],
            dst_ref=buf.at[k],
            send_sem=s_sem.at[k],
            recv_sem=r_sem.at[k],
            device_id=peer(k),
            device_id_type=MESH,
        )

    def flip(r, carry):
        p1t[r] = q1[HALO + r, first:last, :].T
        p2t[r] = q2[HALO + r, first:last, :].T
        return carry

    for stage in range(3):
        size = groups[stage][0]
        for k in range(1, size):
            group_copy(stage, k).start()
        if stage == 0:
            lax.fori_loop(0, rows, flip, 0)
        part = tot[stage]
        for k in range(1, size):
            group_copy(stage, k).wait_recv()
        for k in range(1, size):
            part = part + groups[stage][3][k]
        tot[stage + 1] = part

    mu = []
    for j in range(6):
        mu.append(jnp.broadcast_to(jnp.sum(tot[3, j:j + 1, :], axis=1, keepdims=True), (1, ND)))
    s = jnp.broadcast_to(shift, (1, ND))
    h00 = mu[1] + s * mu[0]
    h01 = mu[2] + s * mu[1]
    h02 = mu[3] + s * mu[2]
    h11 = h02
    h12 = mu[4] + s * mu[3]
    h22 = mu[5] + s * mu[4]
    l10, l20 = h01 / h00, h02 / h00
    d1 = h11 - l10 * h01
    e1 = h12 - l20 * h01
    l21 = e1 / d1
    d2 = h22 - l20 * h02 - l21 * e1
    y1 = mu[1] - l10 * mu[0]
    y2 = mu[2] - l20 * mu[0] - l21 * y1
    c2 = y2 / d2
    c1 = y1 / d1 - l21 * c2
    c0 = mu[0] / h00 - l10 * c1 - l20 * c2

    def store(r):
        return pltpu.make_async_copy(xt.at[r], out_ref.at[:, r, 0, :], store_sem.at[r])

    def combine(r, carry):
        xt[r] = c0 * zt[r] + c1 * p1t[r] + c2 * p2t[r]
        store(r).start()
        return carry
    lax.fori_loop(0, rows, combine, 0)

    for i, (dr, dc) in enumerate(around):
        @pl.when(exists(dr, dc))
        def _():
            halo(i, dr, dc).wait_send()
    for stage in range(3):
        for k in range(1, groups[stage][0]):
            group_copy(stage, k).wait_send()

    def finish(r, carry):
        store(r).wait()
        return carry
    lax.fori_loop(0, rows, finish, 0)


def on_device(grid_rows, grid_cols, depth_rows, phase, pairs):
    m, rows, cols = phase.shape
    total_rows, total_cols = rows + 2 * HALO, cols + 2 * PAD
    y_len = grid_rows // depth_rows
    field = pltpu.VMEM((total_rows, total_cols, ND), F32)
    flat = pltpu.VMEM((rows, ND, cols), F32)
    dma = pltpu.SemaphoreType.DMA
    out = pl.pallas_call(
        lambda *refs: krylov_kernel(grid_rows, grid_cols, depth_rows, *refs),
        name="krylov",
        out_shape=jax.ShapeDtypeStruct((ND, rows, 1, cols), F32),
        in_specs=[pl.BlockSpec(memory_space=pltpu.HBM), pl.BlockSpec(memory_space=pltpu.VMEM)],
        out_specs=pl.BlockSpec(memory_space=pltpu.HBM),
        scratch_shapes=[
            pltpu.VMEM((rows, m, cols), F32),
            field, field, field, field, field,
            flat, flat, flat, flat,
            pltpu.VMEM((2 * ND, 2 * ND), BF16),
            pltpu.VMEM((8, 8, ND), F32),
            pltpu.VMEM((4, 8, ND), F32),
            pltpu.VMEM((grid_cols, 8, ND), F32),
            pltpu.VMEM((y_len, 8, ND), F32),
            pltpu.VMEM((depth_rows, 8, ND), F32),
            pltpu.VMEM((cols + 2 * DIST_COL, ND), F32),
            dma((rows,)), dma((rows,)),
            dma((8,)), dma((8,)),
            dma((grid_cols,)), dma((grid_cols,)),
            dma((y_len,)), dma((y_len,)),
            dma((depth_rows,)), dma((depth_rows,)),
        ],
        compiler_params=pltpu.CompilerParams(
            collective_id=0, has_side_effects=True, vmem_limit_bytes=56 * 1024 * 1024
        ),
    )(phase.reshape(m, rows, 1, cols), pairs.T)
    return out.reshape(ND, rows, cols)


def solution(mesh, depth=8):
    grid_rows, grid_cols = mesh.shape["row"], mesh.shape["col"]

    def body(phase, pairs):
        return on_device(grid_rows, grid_cols, depth, phase, pairs)

    return jax.shard_map(
        body,
        mesh=mesh,
        in_specs=(P(None, "row", "col"), P()),
        out_specs=P(None, "row", "col"),
        check_vma=False,
    )
```

```python
import jax
import jax.numpy as jnp
from jax import lax
from jax.experimental import pallas as pl
from jax.experimental.pallas import tpu as pltpu
from jax.sharding import PartitionSpec as P

ND = 128
LAM2 = 0.8 * 0.8
HALO = 5
PAD = 16
DIST_COL = 8
MESH = pl.DeviceIdType.MESH
F32 = jnp.float32
BF16 = jnp.bfloat16


def split(x, terms):
    parts = []
    for _ in range(terms - 1):
        parts.append(x.astype(BF16))
        x = x - parts[-1].astype(F32)
    return parts + [x.astype(BF16)]


def krylov_kernel(
    grid_rows, grid_cols, depth_rows,
    phase_ref, pairs_hbm, zt, p1t, p2t, weights,
    pairs_ref, ph, z, w1, q1, w2, q2, nmat, acc, tot, in1, in2, cmask,
    pairs_sem, load_sem, halo_send, halo_recv, s1s, s1r, s2s, s2r,
):
    rows, cols = ph.shape[0], ph.shape[2]
    wide = cols + 2 * DIST_COL
    row, col = lax.axis_index("row"), lax.axis_index("col")
    y_len = grid_rows // depth_rows
    row_y, row_z = row // depth_rows, lax.rem(row, depth_rows)

    first, last = PAD, PAD + cols
    total_rows = rows + 2 * HALO

    def clear_sides(e, carry):
        z[e, first - DIST_COL:first, :] = jnp.zeros((DIST_COL, ND), F32)
        z[e, last:last + DIST_COL, :] = jnp.zeros((DIST_COL, ND), F32)
        return carry

    def clear_ends(e, carry):
        for base in (0, HALO + rows):
            z[base + e, first:last, :] = jnp.zeros((cols, ND), F32)
        return carry

    def load(r):
        return pltpu.make_async_copy(phase_ref.at[:, r, 0, :], ph.at[r], load_sem.at[r])

    load_pairs = pltpu.make_async_copy(pairs_hbm, pairs_ref, pairs_sem)
    load_pairs.start()
    strips = [0, rows - 8] + list(range(8, rows - 8, 8))
    for r in range(4):
        load(r).start()

    lax.fori_loop(0, total_rows, clear_sides, 0)
    lax.fori_loop(0, HALO, clear_ends, 0)

    around = [(-1, 0), (1, 0), (0, -1), (0, 1), (-1, -1), (-1, 1), (1, -1), (1, 1)]

    def exists(dr, dc):
        ok = jnp.bool_(True)
        if dr < 0:
            ok = row > 0
        if dr > 0:
            ok = row < grid_rows - 1
        if dc < 0:
            ok = ok & (col > 0)
        if dc > 0:
            ok = ok & (col < grid_cols - 1)
        return ok

    def plane_peer(k):
        other_y = lax.rem(row_y + k // grid_cols, y_len)
        return (other_y * depth_rows + row_z, lax.rem(col + k % grid_cols, grid_cols))

    def z_peer(k):
        return (row_y * depth_rows + lax.rem(row_z + k, depth_rows), col)

    groups = [
        (y_len * grid_cols, plane_peer, in1, s1s, s1r),
        (depth_rows, z_peer, in2, s2s, s2r),
    ]
    barrier = pltpu.get_barrier_semaphore()
    for dr, dc in around:
        @pl.when(exists(dr, dc))
        def _():
            pl.semaphore_signal(barrier, inc=1, device_id=(row + dr, col + dc), device_id_type=MESH)
    for size, peer, _buf, _s, _r in groups:
        for k in range(1, size):
            pl.semaphore_signal(barrier, inc=1, device_id=peer(k), device_id_type=MESH)

    load_pairs.wait()
    for base in strips:
        for r in range(max(base, 4), base + 8):
            load(r).start()
    dates = lax.broadcasted_iota(jnp.int32, (ND, pairs_ref.shape[1]), 0)
    later = (dates == pairs_ref[1:2, :]).astype(F32)
    earlier = (dates == pairs_ref[0:1, :]).astype(F32)
    gt = (later - earlier).astype(BF16)
    normal = lax.dot_general(gt, gt, (((1,), (1,)), ((), ())), preferred_element_type=F32)
    eye = (
        lax.broadcasted_iota(jnp.int32, (ND, ND), 0) == lax.broadcasted_iota(jnp.int32, (ND, ND), 1)
    )
    trace = jnp.sum(jnp.where(eye, normal, 0.0), keepdims=True)
    frob = jnp.sum(normal * normal, keepdims=True)
    shift = jnp.floor(frob / trace + 20.0 * LAM2 + 0.5)
    shifted = normal - jnp.where(eye, shift, 0.0)
    n_hi = shifted.astype(BF16)
    n_lo = (shifted - n_hi.astype(F32)).astype(BF16)
    nmat[...] = jnp.concatenate([n_hi, n_hi, n_hi, n_lo], axis=0)

    side = lax.broadcasted_iota(jnp.int32, (wide, ND), 0)
    left_ok = jnp.where(col > 0, 1.0, 0.0)
    right_ok = jnp.where(col < grid_cols - 1, 1.0, 0.0)
    cmask[...] = jnp.where(
        side < DIST_COL, left_ok, jnp.where(side >= DIST_COL + cols, right_ok, 1.0)
    )
    top_ok = jnp.where(row > 0, 1.0, 0.0)
    bottom_ok = jnp.where(row < grid_rows - 1, 1.0, 0.0)
    def make_z(r):
        parts = []
        for j in range(8):
            load(r + j).wait()
            parts.append(split(ph[r + j], 2))
        for half in (parts[:4], parts[4:]):
            field = sum(
                jnp.dot(gt, jnp.concatenate([p[t] for p in half], axis=1), preferred_element_type=F32)
                for t in range(2)
            )
            for j in range(4):
                part = field[:, j * cols:(j + 1) * cols]
                zt[r + j] = part
                z[HALO + r + j, first:last, :] = part.T
            r = r + 4

    top, low = HALO, rows
    pieces = [(-1, 0, top, HALO + rows, HALO), (1, 0, low, 0, HALO)]
    for dc in (-1, 1):
        pieces += [(-1, dc, top, HALO + rows, HALO - 1), (1, dc, low + 1, 1, HALO - 1)]
    for r in strips:
        pieces += [(0, dc, HALO + r, HALO + r, 8) for dc in (-1, 1)]
    edge_c = {-1: first, 1: last - DIST_COL, 0: first}
    size_c = {-1: DIST_COL, 1: DIST_COL, 0: cols}
    land_c = {-1: last, 1: first - DIST_COL, 0: first}

    def halo(i):
        dr, dc, source, target, count = pieces[i]
        return pltpu.make_async_remote_copy(
            src_ref=z.at[pl.ds(source, count), pl.ds(edge_c[dc], size_c[dc]), :],
            dst_ref=z.at[pl.ds(target, count), pl.ds(land_c[dc], size_c[dc]), :],
            send_sem=halo_send.at[i],
            recv_sem=halo_recv.at[i],
            device_id=(row + dr, col + dc),
            device_id_type=MESH,
        )

    def send(i):
        @pl.when(exists(*pieces[i][:2]))
        def _():
            halo(i).start()

    def arrived(i):
        dr, dc = pieces[i][:2]
        @pl.when(exists(-dr, -dc))
        def _():
            halo(i).wait_recv()

    def sent(i):
        @pl.when(exists(*pieces[i][:2]))
        def _():
            halo(i).wait_send()

    for r in strips[:2]:
        make_z(r)
    n_peers = sum(size - 1 for size, *_ in groups)
    n_around = jnp.int32(0)
    for dr, dc in around:
        n_around = n_around + jnp.where(exists(dr, dc), 1, 0)
    pl.semaphore_wait(barrier, n_around + n_peers)
    for i in range(10):
        send(i)
    for part, r in enumerate(strips[2:]):
        make_z(r)
        for i in (10 + 2 * part, 11 + 2 * part):
            send(i)

    acc[...] = jnp.zeros_like(acc)
    work = pl.ds(PAD - DIST_COL, wide)
    before = pl.ds(PAD - DIST_COL - 1, wide)
    after = pl.ds(PAD - DIST_COL + 1, wide)

    def lap(buf, e):
        beside = buf[e - 1, work, :] + buf[e + 1, work, :] + buf[e, before, :] + buf[e, after, :]
        return 4.0 * buf[e, work, :] - beside

    def normal_times(values):
        pieces = []
        for value in values:
            hi, mid, lo = split(value, 3)
            pieces.append(jnp.concatenate([hi, mid, lo, hi], axis=1))
        height = values[0].shape[0]
        half = (len(values) + 1) // 2
        products = []
        for some in (pieces[:half], pieces[half:]):
            both = jnp.dot(jnp.concatenate(some, axis=0), nmat[...], preferred_element_type=F32)
            products += [both[i * height:(i + 1) * height, :] for i in range(len(some))]
        return products

    def own(value):
        return value[DIST_COL:DIST_COL + cols, :]

    def folded(value):
        return jnp.sum(value.reshape(cols // 8, 8, ND), axis=0)

    def masked(value, scale):
        if scale is None:
            ends = (value[:DIST_COL] * cmask[:DIST_COL], value[-DIST_COL:] * cmask[-DIST_COL:])
            return jnp.concatenate([ends[0], own(value), ends[1]], axis=0)
        return value * (cmask[...] * scale)

    def blocks(lo, hi, block, body):
        if hi - lo == block:
            body(lo)
            return

        def step(i, carry):
            body(lo + block * i)
            return carry
        lax.fori_loop(0, (hi - lo) // block, step, 0)

    def scale_of(e):
        if isinstance(e, int):
            return top_ok if e < HALO else bottom_ok if e >= HALO + rows else None
        return None

    def counts(e):
        return not isinstance(e, int) or HALO <= e < HALO + rows

    def lap_rows(src, dst, lo, hi, block):
        def body(base):
            for e in [base + i for i in range(block)]:
                dst[e, work, :] = masked(lap(src, e), scale_of(e))
        blocks(lo, hi, block, body)

    def k_rows(src, lap_buf, dst, flat, lo, hi, block, moment):
        def body(base):
            es = [base + i for i in range(block)]
            sums = [jnp.zeros((8, ND), F32)] * 3
            products = normal_times([src[e, work, :] for e in es])
            for e, product in zip(es, products):
                value = src[e, work, :]
                result = masked(product + LAM2 * lap(lap_buf, e), scale_of(e))
                dst[e, work, :] = result
                if counts(e):
                    mine, new = own(value), own(result)
                    flat[e - HALO] = new.T
                    if moment == 1:
                        sums[0] = sums[0] + folded(mine * mine)
                    sums[1] = sums[1] + folded(mine * new)
                    sums[2] = sums[2] + folded(new * new)
            if moment == 1:
                acc[0] += sums[0]
            acc[moment] += sums[1]
            acc[moment + 1] += sums[2]
        blocks(lo, hi, block, body)

    def last_rows(lo, hi, block):
        def body(base):
            es = [base + i for i in range(block)]
            products = normal_times([q2[e, first:last, :] for e in es])
            total = jnp.zeros((8, ND), F32)
            for e, product in zip(es, products):
                bent = own(lap(q2, e))
                total = total + folded(q2[e, first:last, :] * product + LAM2 * (bent * bent))
            acc[5] += total
        blocks(lo, hi, block, body)

    for i in range(6, len(pieces)):
        arrived(i)
    lap_rows(z, w1, 6, 36, 3)
    k_rows(z, w1, q1, p1t, 7, 35, 7, 1)
    lap_rows(q1, w2, 8, 34, 2)
    k_rows(q1, w2, q2, p2t, 9, 33, 8, 3)
    last_rows(10, 32, 11)

    for i in range(6):
        arrived(i)
    for lo in (1, 36):
        lap_rows(z, w1, lo, lo + 5, 5)
    for lo in (2, 35):
        k_rows(z, w1, q1, p1t, lo, lo + 5, 5, 1)
    for lo in (3, 34):
        lap_rows(q1, w2, lo, lo + 5, 5)
    for lo in (4, 33):
        k_rows(q1, w2, q2, p2t, lo, lo + 5, 5, 3)
    for lo in (5, 32):
        last_rows(lo, lo + 5, 5)

    lines = jnp.concatenate([jnp.sum(acc[j], axis=0, keepdims=True) for j in range(8)], axis=0)
    lines = jnp.broadcast_to(jnp.sum(lines, axis=1, keepdims=True), (8, ND))
    at = lax.broadcasted_iota(jnp.int32, (8, ND), 0) == lax.broadcasted_iota(jnp.int32, (8, ND), 1)
    tot[0] = jnp.sum(jnp.where(at, lines, 0.0), axis=0, keepdims=True)

    def group_copy(stage, k):
        size, peer, buf, s_sem, r_sem = groups[stage]
        return pltpu.make_async_remote_copy(
            src_ref=tot.at[stage],
            dst_ref=buf.at[k],
            send_sem=s_sem.at[k],
            recv_sem=r_sem.at[k],
            device_id=peer(k),
            device_id_type=MESH,
        )

    for stage in range(2):
        size = groups[stage][0]
        for k in range(1, size):
            group_copy(stage, k).start()
        for k in range(1, size):
            group_copy(stage, k).wait_recv()
        part = tot[stage]
        for k in range(1, size):
            part = part + groups[stage][2][k]
        tot[stage + 1] = part

    lane = lax.broadcasted_iota(jnp.int32, (1, ND), 1)
    mu = []
    for j in range(6):
        mu.append(jnp.broadcast_to(jnp.sum(jnp.where(lane == j, tot[2], 0.0), axis=1, keepdims=True), (1, ND)))
    s = jnp.broadcast_to(shift, (1, ND))
    h00 = mu[1] + s * mu[0]
    h01 = mu[2] + s * mu[1]
    h02 = mu[3] + s * mu[2]
    h11 = h02
    h12 = mu[4] + s * mu[3]
    h22 = mu[5] + s * mu[4]
    l10, l20 = h01 / h00, h02 / h00
    d1 = h11 - l10 * h01
    e1 = h12 - l20 * h01
    l21 = e1 / d1
    d2 = h22 - l20 * h02 - l21 * e1
    y1 = mu[1] - l10 * mu[0]
    y2 = mu[2] - l20 * mu[0] - l21 * y1
    c2 = y2 / d2
    c1 = y1 / d1 - l21 * c2
    c0 = mu[0] / h00 - l10 * c1 - l20 * c2

    weights[...] = jnp.concatenate([c0, c1, c2] + [jnp.zeros((1, ND), F32)] * 5, axis=0)

    for i in range(len(pieces)):
        sent(i)
    for stage in range(2):
        for k in range(1, groups[stage][0]):
            group_copy(stage, k).wait_send()


def store_kernel(zt, p1t, p2t, weights, out_ref, xt, sem):
    rows = zt.shape[0]
    c0, c1, c2 = weights[0:1, :], weights[1:2, :], weights[2:3, :]

    def copy(r):
        return pltpu.make_async_copy(xt.at[r], out_ref.at[:, r, 0, :], sem.at[r])

    def combine(r, carry):
        xt[r] = c0 * zt[r] + c1 * p1t[r] + c2 * p2t[r]
        copy(r).start()
        return carry

    def finish(r, carry):
        copy(r).wait()
        return carry

    lax.fori_loop(0, rows, combine, 0)
    lax.fori_loop(0, rows, finish, 0)


def on_device(grid_rows, grid_cols, depth_rows, phase, pairs):
    m, rows, cols = phase.shape
    total_rows, total_cols = rows + 2 * HALO, cols + 2 * PAD
    y_len = grid_rows // depth_rows
    field = pltpu.VMEM((total_rows, total_cols, ND), F32)
    flat = pltpu.VMEM((rows, ND, cols), F32)
    dma = pltpu.SemaphoreType.DMA
    pieces = 6 + 2 * (rows // 8)
    parts = pl.pallas_call(
        lambda *refs: krylov_kernel(grid_rows, grid_cols, depth_rows, *refs),
        name="krylov",
        out_shape=[jax.ShapeDtypeStruct((rows, ND, cols), F32)] * 3 + [jax.ShapeDtypeStruct((8, ND), F32)],
        in_specs=[pl.BlockSpec(memory_space=pltpu.HBM)] * 2,
        out_specs=[pl.BlockSpec(memory_space=pltpu.VMEM)] * 4,
        scratch_shapes=[
            pltpu.VMEM((2, m), jnp.int32),
            pltpu.VMEM((rows, m, cols), F32),
            field, field, field, field, field,
            pltpu.VMEM((4 * ND, ND), BF16),
            pltpu.VMEM((8, 8, ND), F32),
            pltpu.VMEM((3, 1, ND), F32),
            pltpu.VMEM((y_len * grid_cols, 1, ND), F32),
            pltpu.VMEM((depth_rows, 1, ND), F32),
            pltpu.VMEM((cols + 2 * DIST_COL, ND), F32),
            dma, dma((rows,)),
            dma((pieces,)), dma((pieces,)),
            dma((y_len * grid_cols,)), dma((y_len * grid_cols,)),
            dma((depth_rows,)), dma((depth_rows,)),
        ],
        compiler_params=pltpu.CompilerParams(
            collective_id=0, has_side_effects=True, vmem_limit_bytes=40 * 1024 * 1024
        ),
    )(phase.reshape(m, rows, 1, cols), pltpu.with_memory_space_constraint(pairs.T, pltpu.HBM))
    out = pl.pallas_call(
        store_kernel,
        name="store",
        out_shape=jax.ShapeDtypeStruct((ND, rows, 1, cols), F32),
        in_specs=[pl.BlockSpec(memory_space=pltpu.VMEM)] * 4,
        out_specs=pl.BlockSpec(memory_space=pltpu.HBM),
        scratch_shapes=[flat, dma((rows,))],
        compiler_params=pltpu.CompilerParams(vmem_limit_bytes=16 * 1024 * 1024),
    )(*parts)
    return out.reshape(ND, rows, cols)


def solution(mesh, depth=8):
    grid_rows, grid_cols = mesh.shape["row"], mesh.shape["col"]

    def body(phase, pairs):
        return on_device(grid_rows, grid_cols, depth, phase, pairs)

    return jax.shard_map(
        body,
        mesh=mesh,
        in_specs=(P(None, "row", "col"), P()),
        out_specs=P(None, "row", "col"),
        check_vma=False,
    )
```

```python
import jax
import jax.numpy as jnp
from jax import lax
from jax.experimental import pallas as pl
from jax.experimental.pallas import tpu as pltpu
from jax.sharding import PartitionSpec as P

ND = 128
LAM2 = 0.8 * 0.8
HALO = 5
NEAR = 3
PAD = 16
DIST_COL = 8
MESH = pl.DeviceIdType.MESH
F32 = jnp.float32
BF16 = jnp.bfloat16


def split(x, terms):
    parts = []
    for _ in range(terms - 1):
        parts.append(x.astype(BF16))
        x = x - parts[-1].astype(F32)
    return parts + [x.astype(BF16)]


def krylov_kernel(
    grid_rows, grid_cols, depth_rows,
    phase_ref, pairs_hbm, zt, p1t, p2t, weights,
    pairs_ref, ph, z, w1, q1, w2, q2, nmat, acc, tot, in1, in2,
    pairs_sem, load_sem, halo_send, halo_recv, s1s, s1r, s2s, s2r,
):
    rows, cols = ph.shape[0], ph.shape[2]
    row, col = lax.axis_index("row"), lax.axis_index("col")
    y_len = grid_rows // depth_rows
    row_y, row_z = row // depth_rows, lax.rem(row, depth_rows)

    first, last = PAD, PAD + cols
    total_rows = rows + 2 * HALO

    def clear_sides(e, carry):
        z[e, first - DIST_COL:first, :] = jnp.zeros((DIST_COL, ND), F32)
        z[e, last:last + DIST_COL, :] = jnp.zeros((DIST_COL, ND), F32)
        return carry

    def clear_ends(e, carry):
        for base in (0, HALO + rows):
            z[base + e, first:last, :] = jnp.zeros((cols, ND), F32)
        return carry

    def load(r):
        return pltpu.make_async_copy(phase_ref.at[:, r, 0, :], ph.at[r], load_sem.at[r])

    top_rows, low_rows = range(0, HALO), range(rows - HALO, rows)
    rest = [range(HALO, rows // 2), range(rows // 2, rows - HALO)]
    load_pairs = pltpu.make_async_copy(pairs_hbm, pairs_ref, pairs_sem)
    load_pairs.start()

    around = [(-1, 0), (1, 0), (0, -1), (0, 1), (-1, -1), (-1, 1), (1, -1), (1, 1)]

    def exists(dr, dc):
        ok = jnp.bool_(True)
        if dr < 0:
            ok = row > 0
        if dr > 0:
            ok = row < grid_rows - 1
        if dc < 0:
            ok = ok & (col > 0)
        if dc > 0:
            ok = ok & (col < grid_cols - 1)
        return ok

    def plane_peer(k):
        other_y = lax.rem(row_y + k // grid_cols, y_len)
        return (other_y * depth_rows + row_z, lax.rem(col + k % grid_cols, grid_cols))

    def z_peer(k):
        return (row_y * depth_rows + lax.rem(row_z + k, depth_rows), col)

    groups = [
        (y_len * grid_cols, plane_peer, in1, s1s, s1r),
        (depth_rows, z_peer, in2, s2s, s2r),
    ]
    barrier = pltpu.get_barrier_semaphore()
    for size, peer, _buf, _s, _r in reversed(groups):
        for k in range(1, size):
            pl.semaphore_signal(barrier, inc=1, device_id=peer(k), device_id_type=MESH)
    for part in [top_rows, low_rows] + rest:
        for r in part:
            load(r).start()
    lax.fori_loop(0, total_rows, clear_sides, 0)
    lax.fori_loop(0, HALO, clear_ends, 0)
    for dr, dc in around:
        @pl.when(exists(dr, dc))
        def _():
            pl.semaphore_signal(barrier, inc=1, device_id=(row + dr, col + dc), device_id_type=MESH)

    load_pairs.wait()
    dates = lax.broadcasted_iota(jnp.int32, (ND, pairs_ref.shape[1]), 0)
    later = (dates == pairs_ref[1:2, :]).astype(F32)
    earlier = (dates == pairs_ref[0:1, :]).astype(F32)
    gt = (later - earlier).astype(BF16)
    normal = lax.dot_general(gt, gt, (((1,), (1,)), ((), ())), preferred_element_type=F32)
    eye = (
        lax.broadcasted_iota(jnp.int32, (ND, ND), 0) == lax.broadcasted_iota(jnp.int32, (ND, ND), 1)
    )
    trace = jnp.sum(jnp.where(eye, normal, 0.0), keepdims=True)
    frob = jnp.sum(normal * normal, keepdims=True)
    shift = jnp.floor(frob / trace + 20.0 * LAM2 + 0.5)
    shifted = normal - jnp.where(eye, shift, 0.0)
    n_hi = shifted.astype(BF16)
    n_lo = (shifted - n_hi.astype(F32)).astype(BF16)
    nmat[...] = jnp.concatenate([n_hi, n_hi, n_hi, n_lo], axis=0)

    left_ok = jnp.where(col > 0, 1.0, 0.0)
    right_ok = jnp.where(col < grid_cols - 1, 1.0, 0.0)
    top_ok = jnp.where(row > 0, 1.0, 0.0)
    bottom_ok = jnp.where(row < grid_rows - 1, 1.0, 0.0)
    def make_z(part, group):
        part = list(part)
        for r in part:
            load(r).wait()
        for some in [part[i:i + group] for i in range(0, len(part), group)]:
            terms = [split(ph[r], 2) for r in some]
            field = sum(
                jnp.dot(gt, jnp.concatenate([x[t] for x in terms], axis=1), preferred_element_type=F32)
                for t in range(2)
            )
            for j, r in enumerate(some):
                one = field[:, j * cols:(j + 1) * cols]
                zt[r] = one
                z[HALO + r, first:last, :] = one.T

    far = HALO - NEAR
    top, low, end = HALO, rows + HALO, HALO + rows
    half = rows // 2
    pieces = []
    for dr, source, target in ((-1, top, end), (1, low - NEAR, HALO - NEAR)):
        pieces.append((dr, 0, source, target, NEAR))
        source, target = (top, end) if dr < 0 else (low - HALO + 1, 1)
        pieces += [(dr, dc, source, target, HALO - 1) for dc in (-1, 1)]
        source, target = (top + NEAR, end + NEAR) if dr < 0 else (low - HALO, 0)
        pieces.append((dr, 0, source, target, far))
    for r in (0, half):
        pieces += [(0, dc, HALO + r, HALO + r, half) for dc in (-1, 1)]
    near_pieces, far_pieces, side_pieces = (0, 1, 2, 4, 5, 6), (3, 7), (8, 9, 10, 11)

    def halo(i):
        dr, dc, source, target, count = pieces[i]
        width = cols if dc == 0 else HALO - 1 if dr else DIST_COL
        source_col = last - width if dc == 1 else first
        target_col = {-1: last, 0: first, 1: first - width}[dc]
        return pltpu.make_async_remote_copy(
            src_ref=z.at[pl.ds(source, count), pl.ds(source_col, width), :],
            dst_ref=z.at[pl.ds(target, count), pl.ds(target_col, width), :],
            send_sem=halo_send.at[i],
            recv_sem=halo_recv.at[i],
            device_id=(row + dr, col + dc),
            device_id_type=MESH,
        )

    def send(i):
        @pl.when(exists(*pieces[i][:2]))
        def _():
            halo(i).start()

    def arrived(i):
        dr, dc = pieces[i][:2]
        @pl.when(exists(-dr, -dc))
        def _():
            halo(i).wait_recv()

    def sent(i):
        @pl.when(exists(*pieces[i][:2]))
        def _():
            halo(i).wait_send()

    make_z(top_rows, 5)
    make_z(low_rows, 5)
    make_z(rest[0], 4)
    n_peers = sum(size - 1 for size, *_ in groups)
    n_around = jnp.int32(0)
    for dr, dc in around:
        n_around = n_around + jnp.where(exists(dr, dc), 1, 0)
    pl.semaphore_wait(barrier, n_around + n_peers)
    for i in (0, 4, 1, 2, 5, 6, 3, 7) + side_pieces[:2]:
        send(i)
    make_z(rest[1], 4)
    for i in side_pieces[2:]:
        send(i)

    acc[...] = jnp.zeros_like(acc)

    everything = [(first - DIST_COL, cols + 2 * DIST_COL)]
    own_columns = [(first, cols)]
    inner = [[(first + edge, cols - 2 * edge)] for edge in (8, 16)]
    outer = [[(first - DIST_COL, DIST_COL + edge), (last - edge, DIST_COL + edge)] for edge in (8, 16)]

    def lap(buf, e, span):
        at, width = span
        here = pl.ds(at, width)
        beside = buf[e - 1, here, :] + buf[e + 1, here, :] + buf[e, pl.ds(at - 1, width), :] + buf[e, pl.ds(at + 1, width), :]
        return 4.0 * buf[e, here, :] - beside

    def normal_times(values):
        def times(some):
            pieces = []
            for value in some:
                hi, mid, lo = split(value, 3)
                pieces.append(jnp.concatenate([hi, mid, lo, hi], axis=1))
            both = jnp.dot(jnp.concatenate(pieces, axis=0), nmat[...], preferred_element_type=F32)
            products, at = [], 0
            for value in some:
                products.append(both[at:at + value.shape[0], :])
                at += value.shape[0]
            return products

        half = (len(values) + 1) // 2
        return times(values[:half]) + times(values[half:])

    def own(value, span):
        lo = max(first - span[0], 0)
        return value[lo:lo + min(span[0] + span[1], last) - max(span[0], first), :]

    def folded(value):
        return jnp.sum(value.reshape(value.shape[0] // 8, 8, ND), axis=0)

    def masked(value, span, scale):
        lo, hi = first - span[0], last - span[0]
        parts = [own(value, span)]
        if lo > 0:
            parts = [value[:lo] * left_ok] + parts
        if span[1] > hi:
            parts = parts + [value[hi:] * right_ok]
        value = jnp.concatenate(parts, axis=0) if len(parts) > 1 else parts[0]
        return value if scale is None else value * scale

    def blocks(lo, hi, block, body):
        def step(i, carry):
            body([lo + block * i + j for j in range(block)])
            return carry
        lax.fori_loop(0, (hi - lo) // block, step, 0)

    def scale_of(e):
        if isinstance(e, int):
            return top_ok if e < HALO else bottom_ok if e >= HALO + rows else None
        return None

    def counts(e):
        return not isinstance(e, int) or HALO <= e < HALO + rows

    def lap_rows(src, dst, spans, es):
        for e in es:
            for span in spans:
                dst[e, pl.ds(*span), :] = masked(lap(src, e, span), span, scale_of(e))

    def k_rows(src, lap_buf, dst, flat, moment, spans, es):
        sums = [jnp.zeros((8, ND), F32)] * 3
        places = [(e, span) for e in es for span in spans]
        products = normal_times([src[e, pl.ds(*span), :] for e, span in places])
        for (e, span), product in zip(places, products):
            value = src[e, pl.ds(*span), :]
            result = masked(product + LAM2 * lap(lap_buf, e, span), span, scale_of(e))
            dst[e, pl.ds(*span), :] = result
            if counts(e):
                mine, new = own(value, span), own(result, span)
                if flat is not None:
                    flat[e - HALO] = mine.T
                if moment == 1:
                    sums[0] = sums[0] + folded(mine * mine)
                sums[1] = sums[1] + folded(mine * new)
                sums[2] = sums[2] + folded(new * new)
        if moment == 1:
            acc[0] += sums[0]
        acc[moment] += sums[1]
        acc[moment + 1] += sums[2]

    def last_rows(spans, es):
        (span,) = spans
        products = normal_times([q2[e, pl.ds(*span), :] for e in es])
        total = jnp.zeros((8, ND), F32)
        for e, product in zip(es, products):
            value, bent = q2[e, pl.ds(*span), :], lap(q2, e, span)
            p2t[e - HALO] = value.T
            total = total + folded(value * product + LAM2 * (bent * bent))
        acc[5] += total

    stages = [
        lambda spans, es: lap_rows(z, w1, spans, es),
        lambda spans, es: k_rows(z, w1, q1, None, 1, spans, es),
        lambda spans, es: lap_rows(q1, w2, spans, es),
        lambda spans, es: k_rows(q1, w2, q2, p1t, 3, spans, es),
        last_rows,
    ]
    last_stage = len(stages)
    spans_of = [everything] * (last_stage - 1) + [own_columns]

    def middle(k, spans, block):
        blocks(HALO + k, HALO + rows - k, block, lambda es: stages[k - 1](spans, es))

    middle(1, inner[0], 3)
    middle(2, inner[1], 14)
    for i in side_pieces:
        arrived(i)
    middle(1, outer[0], 6)
    middle(2, outer[1], 14)
    middle(3, everything, 2)
    middle(4, everything, 12)
    middle(5, own_columns, 11)

    def ends(done, ready):
        for k, stage in enumerate(stages, 1):
            above = range(HALO - ready + k, HALO - done + k)
            below = range(HALO + rows + done - k, HALO + rows + ready - k)
            stage(spans_of[k - 1], list(above) + list(below))

    for i in near_pieces:
        arrived(i)
    ends(0, NEAR)
    for i in far_pieces:
        arrived(i)
    ends(NEAR, HALO)

    lines = jnp.concatenate([jnp.sum(acc[j], axis=0, keepdims=True) for j in range(8)], axis=0)
    lines = jnp.broadcast_to(jnp.sum(lines, axis=1, keepdims=True), (8, ND))
    at = lax.broadcasted_iota(jnp.int32, (8, ND), 0) == lax.broadcasted_iota(jnp.int32, (8, ND), 1)
    tot[0] = jnp.sum(jnp.where(at, lines, 0.0), axis=0, keepdims=True)

    def group_copy(stage, k):
        size, peer, buf, s_sem, r_sem = groups[stage]
        return pltpu.make_async_remote_copy(
            src_ref=tot.at[stage],
            dst_ref=buf.at[k],
            send_sem=s_sem.at[k],
            recv_sem=r_sem.at[k],
            device_id=peer(k),
            device_id_type=MESH,
        )

    for stage in range(2):
        size = groups[stage][0]
        for k in range(1, size):
            group_copy(stage, k).start()
        for k in range(1, size):
            group_copy(stage, k).wait_recv()
        part = tot[stage]
        for k in range(1, size):
            part = part + groups[stage][2][k]
        tot[stage + 1] = part

    lane = lax.broadcasted_iota(jnp.int32, (1, ND), 1)
    mu = []
    for j in range(6):
        mu.append(jnp.broadcast_to(jnp.sum(jnp.where(lane == j, tot[2], 0.0), axis=1, keepdims=True), (1, ND)))
    s = jnp.broadcast_to(shift, (1, ND))
    h00 = mu[1] + s * mu[0]
    h01 = mu[2] + s * mu[1]
    h02 = mu[3] + s * mu[2]
    h11 = h02
    h12 = mu[4] + s * mu[3]
    h22 = mu[5] + s * mu[4]
    l10, l20 = h01 / h00, h02 / h00
    d1 = h11 - l10 * h01
    e1 = h12 - l20 * h01
    l21 = e1 / d1
    d2 = h22 - l20 * h02 - l21 * e1
    y1 = mu[1] - l10 * mu[0]
    y2 = mu[2] - l20 * mu[0] - l21 * y1
    c2 = y2 / d2
    c1 = y1 / d1 - l21 * c2
    c0 = mu[0] / h00 - l10 * c1 - l20 * c2

    weights[...] = jnp.concatenate([c0, c1, c2] + [jnp.zeros((1, ND), F32)] * 5, axis=0)

    for i in range(len(pieces)):
        sent(i)
    for stage in range(2):
        for k in range(1, groups[stage][0]):
            group_copy(stage, k).wait_send()


def store_kernel(zt, p1t, p2t, weights, out_ref, xt, sem):
    rows = zt.shape[0]
    c0, c1, c2 = weights[0:1, :], weights[1:2, :], weights[2:3, :]

    def copy(r):
        return pltpu.make_async_copy(xt.at[r], out_ref.at[:, r, 0, :], sem.at[r])

    def combine(r, carry):
        xt[r] = c0 * zt[r] + c1 * p1t[r] + c2 * p2t[r]
        copy(r).start()
        return carry

    def finish(r, carry):
        copy(r).wait()
        return carry

    lax.fori_loop(0, rows, combine, 0)
    lax.fori_loop(0, rows, finish, 0)


def on_device(grid_rows, grid_cols, depth_rows, phase, pairs):
    m, rows, cols = phase.shape
    total_rows, total_cols = rows + 2 * HALO, cols + 2 * PAD
    y_len = grid_rows // depth_rows
    field = pltpu.VMEM((total_rows, total_cols, ND), F32)
    flat = pltpu.VMEM((rows, ND, cols), F32)
    dma = pltpu.SemaphoreType.DMA
    pieces = 12
    parts = pl.pallas_call(
        lambda *refs: krylov_kernel(grid_rows, grid_cols, depth_rows, *refs),
        name="krylov",
        out_shape=[jax.ShapeDtypeStruct((rows, ND, cols), F32)] * 3 + [jax.ShapeDtypeStruct((8, ND), F32)],
        in_specs=[pl.BlockSpec(memory_space=pltpu.HBM)] * 2,
        out_specs=[pl.BlockSpec(memory_space=pltpu.VMEM)] * 4,
        scratch_shapes=[
            pltpu.VMEM((2, m), jnp.int32),
            pltpu.VMEM((rows, m, cols), F32),
            field, field, field, field, field,
            pltpu.VMEM((4 * ND, ND), BF16),
            pltpu.VMEM((8, 8, ND), F32),
            pltpu.VMEM((3, 1, ND), F32),
            pltpu.VMEM((y_len * grid_cols, 1, ND), F32),
            pltpu.VMEM((depth_rows, 1, ND), F32),
            dma, dma((rows,)),
            dma((pieces,)), dma((pieces,)),
            dma((y_len * grid_cols,)), dma((y_len * grid_cols,)),
            dma((depth_rows,)), dma((depth_rows,)),
        ],
        compiler_params=pltpu.CompilerParams(
            collective_id=0, has_side_effects=True, vmem_limit_bytes=40 * 1024 * 1024
        ),
    )(phase.reshape(m, rows, 1, cols), pltpu.with_memory_space_constraint(pairs.T, pltpu.HBM))
    out = pl.pallas_call(
        store_kernel,
        name="store",
        out_shape=jax.ShapeDtypeStruct((ND, rows, 1, cols), F32),
        in_specs=[pl.BlockSpec(memory_space=pltpu.VMEM)] * 4,
        out_specs=pl.BlockSpec(memory_space=pltpu.HBM),
        scratch_shapes=[flat, dma((rows,))],
        compiler_params=pltpu.CompilerParams(vmem_limit_bytes=16 * 1024 * 1024),
    )(*parts)
    return out.reshape(ND, rows, cols)


def solution(mesh, depth=8):
    grid_rows, grid_cols = mesh.shape["row"], mesh.shape["col"]

    def body(phase, pairs):
        return on_device(grid_rows, grid_cols, depth, phase, pairs)

    return jax.shard_map(
        body,
        mesh=mesh,
        in_specs=(P(None, "row", "col"), P()),
        out_specs=P(None, "row", "col"),
        check_vma=False,
    )
```

```python
import jax
import jax.numpy as jnp
from jax import lax
from jax.experimental import pallas as pl
from jax.experimental.pallas import tpu as pltpu
from jax.sharding import PartitionSpec as P

ND = 128
LAM2 = 0.8 * 0.8
HALO = 5
NEAR = 3
PAD = 16
DIST_COL = 8
MESH = pl.DeviceIdType.MESH
F32 = jnp.float32
BF16 = jnp.bfloat16


def split(x, terms):
    parts = []
    for _ in range(terms - 1):
        parts.append(x.astype(BF16))
        x = x - parts[-1].astype(F32)
    return parts + [x.astype(BF16)]


def krylov_kernel(
    grid_rows, grid_cols, depth_rows,
    phase_ref, pairs_hbm, zt, p1t, p2t, weights,
    pairs_ref, ph, z, w1, q1, w2, q2, nmat, acc, tot, in1, in2,
    pairs_sem, load_sem, halo_send, halo_recv, s1s, s1r, s2s, s2r,
):
    rows, cols = ph.shape[0], ph.shape[2]
    row, col = lax.axis_index("row"), lax.axis_index("col")
    y_len = grid_rows // depth_rows
    row_y, row_z = row // depth_rows, lax.rem(row, depth_rows)

    first, last = PAD, PAD + cols
    total_rows = rows + 2 * HALO

    def clear_sides(e, carry):
        z[e, first - DIST_COL:first, :] = jnp.zeros((DIST_COL, ND), F32)
        z[e, last:last + DIST_COL, :] = jnp.zeros((DIST_COL, ND), F32)
        return carry

    def clear_ends(e, carry):
        for base in (0, HALO + rows):
            z[base + e, first:last, :] = jnp.zeros((cols, ND), F32)
        return carry

    def load(r):
        return pltpu.make_async_copy(phase_ref.at[:, r, 0, :], ph.at[r], load_sem.at[r])

    top_rows, low_rows = range(0, HALO), range(rows - HALO, rows)
    rest = [range(HALO, rows // 2), range(rows // 2, rows - HALO)]
    load_pairs = pltpu.make_async_copy(pairs_hbm, pairs_ref, pairs_sem)
    load_pairs.start()

    around = [(-1, 0), (1, 0), (0, -1), (0, 1), (-1, -1), (-1, 1), (1, -1), (1, 1)]

    def exists(dr, dc):
        ok = jnp.bool_(True)
        if dr < 0:
            ok = row > 0
        if dr > 0:
            ok = row < grid_rows - 1
        if dc < 0:
            ok = ok & (col > 0)
        if dc > 0:
            ok = ok & (col < grid_cols - 1)
        return ok

    def plane_peer(k):
        other_y = lax.rem(row_y + k // grid_cols, y_len)
        return (other_y * depth_rows + row_z, lax.rem(col + k % grid_cols, grid_cols))

    def z_peer(k):
        return (row_y * depth_rows + lax.rem(row_z + k, depth_rows), col)

    groups = [
        (y_len * grid_cols, plane_peer, in1, s1s, s1r),
        (depth_rows, z_peer, in2, s2s, s2r),
    ]
    barrier = pltpu.get_barrier_semaphore()
    for size, peer, _buf, _s, _r in reversed(groups):
        for k in range(1, size):
            pl.semaphore_signal(barrier, inc=1, device_id=peer(k), device_id_type=MESH)
    for part in [top_rows, low_rows] + rest:
        for r in part:
            load(r).start()
    lax.fori_loop(0, total_rows, clear_sides, 0)
    lax.fori_loop(0, HALO, clear_ends, 0)
    for dr, dc in around:
        @pl.when(exists(dr, dc))
        def _():
            pl.semaphore_signal(barrier, inc=1, device_id=(row + dr, col + dc), device_id_type=MESH)

    load_pairs.wait()
    dates = lax.broadcasted_iota(jnp.int32, (ND, pairs_ref.shape[1]), 0)
    later = (dates == pairs_ref[1:2, :]).astype(F32)
    earlier = (dates == pairs_ref[0:1, :]).astype(F32)
    gt = (later - earlier).astype(BF16)
    normal = lax.dot_general(gt, gt, (((1,), (1,)), ((), ())), preferred_element_type=F32)
    eye = (
        lax.broadcasted_iota(jnp.int32, (ND, ND), 0) == lax.broadcasted_iota(jnp.int32, (ND, ND), 1)
    )
    trace = jnp.sum(jnp.where(eye, normal, 0.0), keepdims=True)
    frob = jnp.sum(normal * normal, keepdims=True)
    shift = jnp.floor(frob / trace + 20.0 * LAM2 + 0.5)
    shifted = normal - jnp.where(eye, shift, 0.0)
    n_hi = shifted.astype(BF16)
    n_lo = (shifted - n_hi.astype(F32)).astype(BF16)
    nmat[...] = jnp.concatenate([n_hi, n_hi, n_hi, n_lo], axis=0)

    left_ok = jnp.where(col > 0, 1.0, 0.0)
    right_ok = jnp.where(col < grid_cols - 1, 1.0, 0.0)
    top_ok = jnp.where(row > 0, 1.0, 0.0)
    bottom_ok = jnp.where(row < grid_rows - 1, 1.0, 0.0)
    def make_z(part, group):
        part = list(part)
        for r in part:
            load(r).wait()
        for some in [part[i:i + group] for i in range(0, len(part), group)]:
            terms = [split(ph[r], 2) for r in some]
            field = sum(
                jnp.dot(gt, jnp.concatenate([x[t] for x in terms], axis=1), preferred_element_type=F32)
                for t in range(2)
            )
            for j, r in enumerate(some):
                one = field[:, j * cols:(j + 1) * cols]
                zt[r] = one
                z[HALO + r, first:last, :] = one.T

    far = HALO - NEAR
    top, low, end = HALO, rows + HALO, HALO + rows
    half = rows // 2
    pieces = []
    for dr, source, target in ((-1, top, end), (1, low - NEAR, HALO - NEAR)):
        pieces.append((dr, 0, source, target, NEAR))
        source, target = (top, end) if dr < 0 else (low - HALO + 1, 1)
        pieces += [(dr, dc, source, target, HALO - 1) for dc in (-1, 1)]
        source, target = (top + NEAR, end + NEAR) if dr < 0 else (low - HALO, 0)
        pieces.append((dr, 0, source, target, far))
    for r in (0, half):
        pieces += [(0, dc, HALO + r, HALO + r, half) for dc in (-1, 1)]
    near_pieces, far_pieces, side_pieces = (0, 1, 2, 4, 5, 6), (3, 7), (8, 9, 10, 11)

    def halo(i):
        dr, dc, source, target, count = pieces[i]
        width = cols if dc == 0 else HALO - 1 if dr else HALO
        source_col = last - width if dc == 1 else first
        target_col = {-1: last, 0: first, 1: first - width}[dc]
        return pltpu.make_async_remote_copy(
            src_ref=z.at[pl.ds(source, count), pl.ds(source_col, width), :],
            dst_ref=z.at[pl.ds(target, count), pl.ds(target_col, width), :],
            send_sem=halo_send.at[i],
            recv_sem=halo_recv.at[i],
            device_id=(row + dr, col + dc),
            device_id_type=MESH,
        )

    def send(i):
        @pl.when(exists(*pieces[i][:2]))
        def _():
            halo(i).start()

    def arrived(i):
        dr, dc = pieces[i][:2]
        @pl.when(exists(-dr, -dc))
        def _():
            halo(i).wait_recv()

    def sent(i):
        @pl.when(exists(*pieces[i][:2]))
        def _():
            halo(i).wait_send()

    make_z(top_rows, 5)
    make_z(low_rows, 5)
    n_peers = sum(size - 1 for size, *_ in groups)
    n_around = jnp.int32(0)
    for dr, dc in around:
        n_around = n_around + jnp.where(exists(dr, dc), 1, 0)
    pl.semaphore_wait(barrier, n_around + n_peers)
    for i in (0, 4, 1, 2, 5, 6, 3, 7):
        send(i)
    for part, side in zip(rest, (side_pieces[:2], side_pieces[2:])):
        make_z(part, 4)
        for i in side:
            send(i)

    acc[...] = jnp.zeros_like(acc)

    everything = [(first - DIST_COL, cols + 2 * DIST_COL)]
    own_columns = [(first, cols)]
    inner = [[(first + edge, cols - 2 * edge)] for edge in (8, 16, 24, 32)]
    outer = [[(first - DIST_COL, DIST_COL + edge), (last - edge, DIST_COL + edge)] for edge in (8, 16, 24, 32)]

    def lap(buf, e, span):
        at, width = span
        here = pl.ds(at, width)
        beside = buf[e - 1, here, :] + buf[e + 1, here, :] + buf[e, pl.ds(at - 1, width), :] + buf[e, pl.ds(at + 1, width), :]
        return 4.0 * buf[e, here, :] - beside

    def normal_times(values):
        def times(some):
            pieces = []
            for value in some:
                hi, mid, lo = split(value, 3)
                pieces.append(jnp.concatenate([hi, mid, lo, hi], axis=1))
            both = jnp.dot(jnp.concatenate(pieces, axis=0), nmat[...], preferred_element_type=F32)
            products, at = [], 0
            for value in some:
                products.append(both[at:at + value.shape[0], :])
                at += value.shape[0]
            return products

        half = (len(values) + 1) // 2
        return times(values[:half]) + times(values[half:])

    def own(value, span):
        lo = max(first - span[0], 0)
        return value[lo:lo + min(span[0] + span[1], last) - max(span[0], first), :]

    def folded(value):
        return jnp.sum(value.reshape(value.shape[0] // 8, 8, ND), axis=0)

    def masked(value, span, scale):
        lo, hi = first - span[0], last - span[0]
        parts = [own(value, span)]
        if lo > 0:
            parts = [value[:lo] * left_ok] + parts
        if span[1] > hi:
            parts = parts + [value[hi:] * right_ok]
        value = jnp.concatenate(parts, axis=0) if len(parts) > 1 else parts[0]
        return value if scale is None else value * scale

    def blocks(lo, hi, block, body):
        def step(i, carry):
            body([lo + block * i + j for j in range(block)])
            return carry
        lax.fori_loop(0, (hi - lo) // block, step, 0)

    def scale_of(e):
        if isinstance(e, int):
            return top_ok if e < HALO else bottom_ok if e >= HALO + rows else None
        return None

    def counts(e):
        return not isinstance(e, int) or HALO <= e < HALO + rows

    def lap_rows(src, dst, spans, es):
        for e in es:
            for span in spans:
                dst[e, pl.ds(*span), :] = masked(lap(src, e, span), span, scale_of(e))

    def k_rows(src, lap_buf, dst, moment, spans, es):
        sums = [jnp.zeros((8, ND), F32)] * 3
        places = [(e, span) for e in es for span in spans]
        products = normal_times([src[e, pl.ds(*span), :] for e, span in places])
        for (e, span), product in zip(places, products):
            value = src[e, pl.ds(*span), :]
            result = masked(product + LAM2 * lap(lap_buf, e, span), span, scale_of(e))
            dst[e, pl.ds(*span), :] = result
            if counts(e):
                mine, new = own(value, span), own(result, span)
                if moment == 1:
                    sums[0] = sums[0] + folded(mine * mine)
                sums[1] = sums[1] + folded(mine * new)
                sums[2] = sums[2] + folded(new * new)
        if moment == 1:
            acc[0] += sums[0]
        acc[moment] += sums[1]
        acc[moment + 1] += sums[2]

    def last_rows(spans, es):
        (span,) = spans
        products = normal_times([q2[e, pl.ds(*span), :] for e in es])
        total = jnp.zeros((8, ND), F32)
        for e, product in zip(es, products):
            value, bent = q2[e, pl.ds(*span), :], lap(q2, e, span)
            p1t[e - HALO] = q1[e, first:last, :].T
            p2t[e - HALO] = value.T
            total = total + folded(value * product + LAM2 * (bent * bent))
        acc[5] += total

    stages = [
        lambda spans, es: lap_rows(z, w1, spans, es),
        lambda spans, es: k_rows(z, w1, q1, 1, spans, es),
        lambda spans, es: lap_rows(q1, w2, spans, es),
        lambda spans, es: k_rows(q1, w2, q2, 3, spans, es),
        last_rows,
    ]
    last_stage = len(stages)
    spans_of = [everything] * (last_stage - 1) + [own_columns]

    def middle(k, spans, block):
        blocks(HALO + k, HALO + rows - k, block, lambda es: stages[k - 1](spans, es))

    for k, block in enumerate((3, 14, 2, 12), 1):
        middle(k, inner[k - 1], block)
    for i in side_pieces:
        arrived(i)
    for k, block in enumerate((6, 14, 2, 12), 1):
        middle(k, outer[k - 1], block)
    middle(5, own_columns, 11)

    def ends(done, ready):
        for k, stage in enumerate(stages, 1):
            above = range(HALO - ready + k, HALO - done + k)
            below = range(HALO + rows + done - k, HALO + rows + ready - k)
            stage(spans_of[k - 1], list(above) + list(below))

    for i in near_pieces:
        arrived(i)
    ends(0, NEAR)
    for i in far_pieces:
        arrived(i)
    ends(NEAR, HALO)

    lines = jnp.concatenate([jnp.sum(acc[j], axis=0, keepdims=True) for j in range(8)], axis=0)
    lines = jnp.broadcast_to(jnp.sum(lines, axis=1, keepdims=True), (8, ND))
    at = lax.broadcasted_iota(jnp.int32, (8, ND), 0) == lax.broadcasted_iota(jnp.int32, (8, ND), 1)
    tot[0] = jnp.sum(jnp.where(at, lines, 0.0), axis=0, keepdims=True)

    def group_copy(stage, k):
        size, peer, buf, s_sem, r_sem = groups[stage]
        return pltpu.make_async_remote_copy(
            src_ref=tot.at[stage],
            dst_ref=buf.at[k],
            send_sem=s_sem.at[k],
            recv_sem=r_sem.at[k],
            device_id=peer(k),
            device_id_type=MESH,
        )

    for stage in range(2):
        size = groups[stage][0]
        for k in range(1, size):
            group_copy(stage, k).start()
        for k in range(1, size):
            group_copy(stage, k).wait_recv()
        part = tot[stage]
        for k in range(1, size):
            part = part + groups[stage][2][k]
        tot[stage + 1] = part

    lane = lax.broadcasted_iota(jnp.int32, (1, ND), 1)
    mu = []
    for j in range(6):
        mu.append(jnp.broadcast_to(jnp.sum(jnp.where(lane == j, tot[2], 0.0), axis=1, keepdims=True), (1, ND)))
    s = jnp.broadcast_to(shift, (1, ND))
    h00 = mu[1] + s * mu[0]
    h01 = mu[2] + s * mu[1]
    h02 = mu[3] + s * mu[2]
    h11 = h02
    h12 = mu[4] + s * mu[3]
    h22 = mu[5] + s * mu[4]
    l10, l20 = h01 / h00, h02 / h00
    d1 = h11 - l10 * h01
    e1 = h12 - l20 * h01
    l21 = e1 / d1
    d2 = h22 - l20 * h02 - l21 * e1
    y1 = mu[1] - l10 * mu[0]
    y2 = mu[2] - l20 * mu[0] - l21 * y1
    c2 = y2 / d2
    c1 = y1 / d1 - l21 * c2
    c0 = mu[0] / h00 - l10 * c1 - l20 * c2

    weights[...] = jnp.concatenate([c0, c1, c2] + [jnp.zeros((1, ND), F32)] * 5, axis=0)

    for i in range(len(pieces)):
        sent(i)
    for stage in range(2):
        for k in range(1, groups[stage][0]):
            group_copy(stage, k).wait_send()


def store_kernel(zt, p1t, p2t, weights, out_ref, xt, sem):
    rows = zt.shape[0]
    c0, c1, c2 = weights[0:1, :], weights[1:2, :], weights[2:3, :]

    def copy(r):
        return pltpu.make_async_copy(xt.at[r], out_ref.at[:, r, 0, :], sem.at[r])

    def combine(r, carry):
        xt[r] = c0 * zt[r] + c1 * p1t[r] + c2 * p2t[r]
        copy(r).start()
        return carry

    def finish(r, carry):
        copy(r).wait()
        return carry

    lax.fori_loop(0, rows, combine, 0)
    lax.fori_loop(0, rows, finish, 0)


def on_device(grid_rows, grid_cols, depth_rows, phase, pairs):
    m, rows, cols = phase.shape
    total_rows, total_cols = rows + 2 * HALO, cols + 2 * PAD
    y_len = grid_rows // depth_rows
    field = pltpu.VMEM((total_rows, total_cols, ND), F32)
    flat = pltpu.VMEM((rows, ND, cols), F32)
    dma = pltpu.SemaphoreType.DMA
    pieces = 12
    parts = pl.pallas_call(
        lambda *refs: krylov_kernel(grid_rows, grid_cols, depth_rows, *refs),
        name="krylov",
        out_shape=[jax.ShapeDtypeStruct((rows, ND, cols), F32)] * 3 + [jax.ShapeDtypeStruct((8, ND), F32)],
        in_specs=[pl.BlockSpec(memory_space=pltpu.HBM)] * 2,
        out_specs=[pl.BlockSpec(memory_space=pltpu.VMEM)] * 4,
        scratch_shapes=[
            pltpu.VMEM((2, m), jnp.int32),
            pltpu.VMEM((rows, m, cols), F32),
            field, field, field, field, field,
            pltpu.VMEM((4 * ND, ND), BF16),
            pltpu.VMEM((8, 8, ND), F32),
            pltpu.VMEM((3, 1, ND), F32),
            pltpu.VMEM((y_len * grid_cols, 1, ND), F32),
            pltpu.VMEM((depth_rows, 1, ND), F32),
            dma, dma((rows,)),
            dma((pieces,)), dma((pieces,)),
            dma((y_len * grid_cols,)), dma((y_len * grid_cols,)),
            dma((depth_rows,)), dma((depth_rows,)),
        ],
        compiler_params=pltpu.CompilerParams(
            collective_id=0, has_side_effects=True, vmem_limit_bytes=40 * 1024 * 1024
        ),
    )(phase.reshape(m, rows, 1, cols), pltpu.with_memory_space_constraint(pairs.T, pltpu.HBM))
    out = pl.pallas_call(
        store_kernel,
        name="store",
        out_shape=jax.ShapeDtypeStruct((ND, rows, 1, cols), F32),
        in_specs=[pl.BlockSpec(memory_space=pltpu.VMEM)] * 4,
        out_specs=pl.BlockSpec(memory_space=pltpu.HBM),
        scratch_shapes=[flat, dma((rows,))],
        compiler_params=pltpu.CompilerParams(vmem_limit_bytes=16 * 1024 * 1024),
    )(*parts)
    return out.reshape(ND, rows, cols)


def solution(mesh, depth=8):
    grid_rows, grid_cols = mesh.shape["row"], mesh.shape["col"]

    def body(phase, pairs):
        return on_device(grid_rows, grid_cols, depth, phase, pairs)

    return jax.shard_map(
        body,
        mesh=mesh,
        in_specs=(P(None, "row", "col"), P()),
        out_specs=P(None, "row", "col"),
        check_vma=False,
    )
```

```python
import jax
import jax.numpy as jnp
from jax import lax
from jax.experimental import pallas as pl
from jax.experimental.pallas import tpu as pltpu
from jax.sharding import PartitionSpec as P

ND = 128
LAM2 = 0.8 * 0.8
HALO = 5
NEAR = 3
PAD = 16
DIST_COL = 8
MESH = pl.DeviceIdType.MESH
F32 = jnp.float32
BF16 = jnp.bfloat16


def split(x, terms):
    parts = []
    for _ in range(terms - 1):
        parts.append(x.astype(BF16))
        x = x - parts[-1].astype(F32)
    return parts + [x.astype(BF16)]


def krylov_kernel(
    grid_rows, grid_cols, depth_rows,
    phase_ref, pairs_hbm, zt, p1t, p2t, weights,
    pairs_ref, ph, z, w1, q1, w2, q2, nmat, acc, tot, in1, in2,
    pairs_sem, load_sem, halo_send, halo_recv, s1s, s1r, s2s, s2r,
):
    rows, cols = ph.shape[0], ph.shape[2]
    row, col = lax.axis_index("row"), lax.axis_index("col")
    y_len = grid_rows // depth_rows
    row_y, row_z = row // depth_rows, lax.rem(row, depth_rows)

    first, last = PAD, PAD + cols
    total_rows = rows + 2 * HALO

    def clear_sides(e, carry):
        z[e, first - DIST_COL:first, :] = jnp.zeros((DIST_COL, ND), F32)
        z[e, last:last + DIST_COL, :] = jnp.zeros((DIST_COL, ND), F32)
        return carry

    def clear_ends(e, carry):
        for base in (0, HALO + rows):
            z[base + e, first:last, :] = jnp.zeros((cols, ND), F32)
        return carry

    def load(i, r):
        return pltpu.make_async_copy(phase_ref.at[:, r, 0, :], ph.at[r], load_sem.at[i])

    def loaded(i):
        here = ph.at[pl.ds(parts[i].start, len(parts[i]))]
        pltpu.make_async_copy(here, here, load_sem.at[i]).wait()

    top_rows, low_rows = range(0, HALO), range(rows - HALO, rows)
    parts = [top_rows, low_rows, range(HALO, rows // 2), range(rows // 2, rows - HALO)]
    load_pairs = pltpu.make_async_copy(pairs_hbm, pairs_ref, pairs_sem)
    load_pairs.start()
    for r in top_rows:
        load(0, r).start()

    around = [(-1, 0), (1, 0), (0, -1), (0, 1), (-1, -1), (-1, 1), (1, -1), (1, 1)]

    def exists(dr, dc):
        ok = jnp.bool_(True)
        if dr < 0:
            ok = row > 0
        if dr > 0:
            ok = row < grid_rows - 1
        if dc < 0:
            ok = ok & (col > 0)
        if dc > 0:
            ok = ok & (col < grid_cols - 1)
        return ok

    def plane_peer(k):
        other_y = lax.rem(row_y + k // grid_cols, y_len)
        return (other_y * depth_rows + row_z, lax.rem(col + k % grid_cols, grid_cols))

    def z_peer(k):
        return (row_y * depth_rows + lax.rem(row_z + k, depth_rows), col)

    groups = [
        (y_len * grid_cols, plane_peer, in1, s1s, s1r),
        (depth_rows, z_peer, in2, s2s, s2r),
    ]
    barrier = pltpu.get_barrier_semaphore()
    for size, peer, _buf, _s, _r in reversed(groups):
        for k in range(1, size):
            pl.semaphore_signal(barrier, inc=1, device_id=peer(k), device_id_type=MESH)
    for i in (1, 2, 3):
        for r in parts[i]:
            load(i, r).start()
    lax.fori_loop(0, total_rows, clear_sides, 0)
    lax.fori_loop(0, HALO, clear_ends, 0)
    for dr, dc in around:
        @pl.when(exists(dr, dc))
        def _():
            pl.semaphore_signal(barrier, inc=1, device_id=(row + dr, col + dc), device_id_type=MESH)

    load_pairs.wait()
    dates = lax.broadcasted_iota(jnp.int32, (ND, pairs_ref.shape[1]), 0)
    later = (dates == pairs_ref[1:2, :]).astype(F32)
    earlier = (dates == pairs_ref[0:1, :]).astype(F32)
    gt = (later - earlier).astype(BF16)
    normal = lax.dot_general(gt, gt, (((1,), (1,)), ((), ())), preferred_element_type=F32)
    eye = (
        lax.broadcasted_iota(jnp.int32, (ND, ND), 0) == lax.broadcasted_iota(jnp.int32, (ND, ND), 1)
    )
    trace = jnp.sum(jnp.where(eye, normal, 0.0), keepdims=True)
    frob = jnp.sum(normal * normal, keepdims=True)
    shift = jnp.floor(frob / trace + 20.0 * LAM2 + 0.5)
    shifted = normal - jnp.where(eye, shift, 0.0)
    n_hi = shifted.astype(BF16)
    n_lo = (shifted - n_hi.astype(F32)).astype(BF16)
    nmat[...] = jnp.concatenate([n_hi, n_hi, n_hi, n_lo], axis=0)

    left_ok = jnp.where(col > 0, 1.0, 0.0)
    right_ok = jnp.where(col < grid_cols - 1, 1.0, 0.0)
    top_ok = jnp.where(row > 0, 1.0, 0.0)
    bottom_ok = jnp.where(row < grid_rows - 1, 1.0, 0.0)
    def make_z(i, group):
        part = list(parts[i])
        loaded(i)
        for some in [part[at:at + group] for at in range(0, len(part), group)]:
            terms = [split(ph[r], 2) for r in some]
            field = sum(
                jnp.dot(gt, jnp.concatenate([x[t] for x in terms], axis=1), preferred_element_type=F32)
                for t in range(2)
            )
            for j, r in enumerate(some):
                one = field[:, j * cols:(j + 1) * cols]
                zt[r] = one
                z[HALO + r, first:last, :] = one.T

    far = HALO - NEAR
    top, low, end = HALO, rows + HALO, HALO + rows
    half = rows // 2
    pieces = []
    for dr, source, target in ((-1, top, end), (1, low - NEAR, HALO - NEAR)):
        pieces.append((dr, 0, source, target, NEAR))
        source, target = (top, end) if dr < 0 else (low - HALO + 1, 1)
        pieces += [(dr, dc, source, target, HALO - 1) for dc in (-1, 1)]
        source, target = (top + NEAR, end + NEAR) if dr < 0 else (low - HALO, 0)
        pieces.append((dr, 0, source, target, far))
    for r in (0, half):
        pieces += [(0, dc, HALO + r, HALO + r, half) for dc in (-1, 1)]
    near_pieces, far_pieces, side_pieces = (0, 1, 2, 4, 5, 6), (3, 7), (8, 9, 10, 11)

    def halo(i):
        dr, dc, source, target, count = pieces[i]
        width = cols if dc == 0 else HALO - 1 if dr else HALO
        source_col = last - width if dc == 1 else first
        target_col = {-1: last, 0: first, 1: first - width}[dc]
        return pltpu.make_async_remote_copy(
            src_ref=z.at[pl.ds(source, count), pl.ds(source_col, width), :],
            dst_ref=z.at[pl.ds(target, count), pl.ds(target_col, width), :],
            send_sem=halo_send.at[i],
            recv_sem=halo_recv.at[i],
            device_id=(row + dr, col + dc),
            device_id_type=MESH,
        )

    def send(i):
        @pl.when(exists(*pieces[i][:2]))
        def _():
            halo(i).start()

    def arrived(i):
        dr, dc = pieces[i][:2]
        @pl.when(exists(-dr, -dc))
        def _():
            halo(i).wait_recv()

    def sent(i):
        @pl.when(exists(*pieces[i][:2]))
        def _():
            halo(i).wait_send()

    make_z(0, 5)
    make_z(1, 5)
    n_peers = sum(size - 1 for size, *_ in groups)
    n_around = jnp.int32(0)
    for dr, dc in around:
        n_around = n_around + jnp.where(exists(dr, dc), 1, 0)
    pl.semaphore_wait(barrier, n_around + n_peers)
    for i in (0, 4, 1, 2, 5, 6, 3, 7):
        send(i)
    for part, side in ((2, side_pieces[:2]), (3, side_pieces[2:])):
        make_z(part, 4)
        for i in side:
            send(i)

    acc[...] = jnp.zeros_like(acc)

    everything = [(first - DIST_COL, cols + 2 * DIST_COL)]
    own_columns = [(first, cols)]
    inner = [[(first + edge, cols - 2 * edge)] for edge in (8, 16, 24, 32)]
    outer = [[(first - DIST_COL, DIST_COL + edge), (last - edge, DIST_COL + edge)] for edge in (8, 16, 24, 32)]

    def lap(buf, e, span):
        at, width = span
        here = pl.ds(at, width)
        beside = buf[e - 1, here, :] + buf[e + 1, here, :] + buf[e, pl.ds(at - 1, width), :] + buf[e, pl.ds(at + 1, width), :]
        return 4.0 * buf[e, here, :] - beside

    def normal_times(values):
        def times(some):
            pieces = []
            for value in some:
                hi, mid, lo = split(value, 3)
                pieces.append(jnp.concatenate([hi, mid, lo, hi], axis=1))
            both = jnp.dot(jnp.concatenate(pieces, axis=0), nmat[...], preferred_element_type=F32)
            products, at = [], 0
            for value in some:
                products.append(both[at:at + value.shape[0], :])
                at += value.shape[0]
            return products

        half = (len(values) + 1) // 2
        return times(values[:half]) + times(values[half:])

    def own(value, span):
        lo = max(first - span[0], 0)
        return value[lo:lo + min(span[0] + span[1], last) - max(span[0], first), :]

    def folded(value):
        return jnp.sum(value.reshape(value.shape[0] // 8, 8, ND), axis=0)

    def masked(value, span, scale):
        lo, hi = first - span[0], last - span[0]
        parts = [own(value, span)]
        if lo > 0:
            parts = [value[:lo] * left_ok] + parts
        if span[1] > hi:
            parts = parts + [value[hi:] * right_ok]
        value = jnp.concatenate(parts, axis=0) if len(parts) > 1 else parts[0]
        return value if scale is None else value * scale

    def blocks(lo, hi, block, body):
        def step(i, carry):
            body([lo + block * i + j for j in range(block)])
            return carry
        lax.fori_loop(0, (hi - lo) // block, step, 0)

    def scale_of(e):
        if isinstance(e, int):
            return top_ok if e < HALO else bottom_ok if e >= HALO + rows else None
        return None

    def counts(e):
        return not isinstance(e, int) or HALO <= e < HALO + rows

    def lap_rows(src, dst, spans, es):
        for e in es:
            for span in spans:
                dst[e, pl.ds(*span), :] = masked(lap(src, e, span), span, scale_of(e))

    def k_rows(src, lap_buf, dst, moment, spans, es):
        sums = [jnp.zeros((8, ND), F32)] * 3
        places = [(e, span) for e in es for span in spans]
        products = normal_times([src[e, pl.ds(*span), :] for e, span in places])
        for (e, span), product in zip(places, products):
            value = src[e, pl.ds(*span), :]
            result = masked(product + LAM2 * lap(lap_buf, e, span), span, scale_of(e))
            dst[e, pl.ds(*span), :] = result
            if counts(e):
                mine, new = own(value, span), own(result, span)
                if moment == 1:
                    sums[0] = sums[0] + folded(mine * mine)
                sums[1] = sums[1] + folded(mine * new)
                sums[2] = sums[2] + folded(new * new)
        if moment == 1:
            acc[0] += sums[0]
        acc[moment] += sums[1]
        acc[moment + 1] += sums[2]

    def last_rows(spans, es):
        (span,) = spans
        products = normal_times([q2[e, pl.ds(*span), :] for e in es])
        total = jnp.zeros((8, ND), F32)
        for e, product in zip(es, products):
            value, bent = q2[e, pl.ds(*span), :], lap(q2, e, span)
            p1t[e - HALO] = q1[e, first:last, :].T
            p2t[e - HALO] = value.T
            total = total + folded(value * product + LAM2 * (bent * bent))
        acc[5] += total

    stages = [
        lambda spans, es: lap_rows(z, w1, spans, es),
        lambda spans, es: k_rows(z, w1, q1, 1, spans, es),
        lambda spans, es: lap_rows(q1, w2, spans, es),
        lambda spans, es: k_rows(q1, w2, q2, 3, spans, es),
        last_rows,
    ]
    last_stage = len(stages)
    spans_of = [everything] * (last_stage - 1) + [own_columns]

    def middle(k, spans, block):
        blocks(HALO + k, HALO + rows - k, block, lambda es: stages[k - 1](spans, es))

    for k, block in enumerate((3, 14, 2, 12), 1):
        middle(k, inner[k - 1], block)
    for i in side_pieces:
        arrived(i)
    for k, block in enumerate((6, 14, 2, 12), 1):
        middle(k, outer[k - 1], block)
    middle(5, own_columns, 11)

    def ends(done, ready):
        for k, stage in enumerate(stages, 1):
            above = range(HALO - ready + k, HALO - done + k)
            below = range(HALO + rows + done - k, HALO + rows + ready - k)
            stage(spans_of[k - 1], list(above) + list(below))

    for i in near_pieces:
        arrived(i)
    ends(0, NEAR)
    for i in far_pieces:
        arrived(i)
    ends(NEAR, HALO)

    lines = jnp.concatenate([jnp.sum(acc[j], axis=0, keepdims=True) for j in range(8)], axis=0)
    lines = jnp.broadcast_to(jnp.sum(lines, axis=1, keepdims=True), (8, ND))
    at = lax.broadcasted_iota(jnp.int32, (8, ND), 0) == lax.broadcasted_iota(jnp.int32, (8, ND), 1)
    tot[0] = jnp.sum(jnp.where(at, lines, 0.0), axis=0, keepdims=True)

    def group_copy(stage, k):
        size, peer, buf, s_sem, r_sem = groups[stage]
        return pltpu.make_async_remote_copy(
            src_ref=tot.at[stage],
            dst_ref=buf.at[k],
            send_sem=s_sem,
            recv_sem=r_sem,
            device_id=peer(k),
            device_id_type=MESH,
        )

    def all_copies(stage):
        size, peer, buf, s_sem, r_sem = groups[stage]
        others = buf.at[pl.ds(1, size - 1)]
        return pltpu.make_async_remote_copy(
            src_ref=others, dst_ref=others, send_sem=s_sem, recv_sem=r_sem, device_id=peer(1), device_id_type=MESH
        )

    for stage in range(2):
        size = groups[stage][0]
        for k in range(1, size):
            group_copy(stage, k).start()
        if stage == 0:
            for i in range(len(pieces)):
                sent(i)
        all_copies(stage).wait_send()
        all_copies(stage).wait_recv()
        part = tot[stage]
        for k in range(1, size):
            part = part + groups[stage][2][k]
        tot[stage + 1] = part

    lane = lax.broadcasted_iota(jnp.int32, (1, ND), 1)
    mu = []
    for j in range(6):
        mu.append(jnp.broadcast_to(jnp.sum(jnp.where(lane == j, tot[2], 0.0), axis=1, keepdims=True), (1, ND)))
    s = jnp.broadcast_to(shift, (1, ND))
    h00 = mu[1] + s * mu[0]
    h01 = mu[2] + s * mu[1]
    h02 = mu[3] + s * mu[2]
    h11 = h02
    h12 = mu[4] + s * mu[3]
    h22 = mu[5] + s * mu[4]
    l10, l20 = h01 / h00, h02 / h00
    d1 = h11 - l10 * h01
    e1 = h12 - l20 * h01
    l21 = e1 / d1
    d2 = h22 - l20 * h02 - l21 * e1
    y1 = mu[1] - l10 * mu[0]
    y2 = mu[2] - l20 * mu[0] - l21 * y1
    c2 = y2 / d2
    c1 = y1 / d1 - l21 * c2
    c0 = mu[0] / h00 - l10 * c1 - l20 * c2

    weights[...] = jnp.concatenate([c0, c1, c2] + [jnp.zeros((1, ND), F32)] * 5, axis=0)


def store_kernel(zt, p1t, p2t, weights, out_ref, xt, sem):
    rows = zt.shape[0]
    c0, c1, c2 = weights[0:1, :], weights[1:2, :], weights[2:3, :]

    def copy(r):
        return pltpu.make_async_copy(xt.at[r], out_ref.at[:, r, 0, :], sem)

    def combine(r, carry):
        xt[r] = c0 * zt[r] + c1 * p1t[r] + c2 * p2t[r]
        copy(r).start()
        return carry

    lax.fori_loop(0, rows, combine, 0)
    pltpu.make_async_copy(xt, xt, sem).wait()


def on_device(grid_rows, grid_cols, depth_rows, phase, pairs):
    m, rows, cols = phase.shape
    total_rows, total_cols = rows + 2 * HALO, cols + 2 * PAD
    y_len = grid_rows // depth_rows
    field = pltpu.VMEM((total_rows, total_cols, ND), F32)
    flat = pltpu.VMEM((rows, ND, cols), F32)
    dma = pltpu.SemaphoreType.DMA
    pieces = 12
    parts = pl.pallas_call(
        lambda *refs: krylov_kernel(grid_rows, grid_cols, depth_rows, *refs),
        name="krylov",
        out_shape=[jax.ShapeDtypeStruct((rows, ND, cols), F32)] * 3 + [jax.ShapeDtypeStruct((8, ND), F32)],
        in_specs=[pl.BlockSpec(memory_space=pltpu.HBM)] * 2,
        out_specs=[pl.BlockSpec(memory_space=pltpu.VMEM)] * 4,
        scratch_shapes=[
            pltpu.VMEM((2, m), jnp.int32),
            pltpu.VMEM((rows, m, cols), F32),
            field, field, field, field, field,
            pltpu.VMEM((4 * ND, ND), BF16),
            pltpu.VMEM((8, 8, ND), F32),
            pltpu.VMEM((3, 1, ND), F32),
            pltpu.VMEM((y_len * grid_cols, 1, ND), F32),
            pltpu.VMEM((depth_rows, 1, ND), F32),
            dma, dma((4,)),
            dma((pieces,)), dma((pieces,)),
            dma, dma, dma, dma,
        ],
        compiler_params=pltpu.CompilerParams(
            collective_id=0, has_side_effects=True, vmem_limit_bytes=40 * 1024 * 1024
        ),
    )(phase.reshape(m, rows, 1, cols), pltpu.with_memory_space_constraint(pairs.T, pltpu.HBM))
    out = pl.pallas_call(
        store_kernel,
        name="store",
        out_shape=jax.ShapeDtypeStruct((ND, rows, 1, cols), F32),
        in_specs=[pl.BlockSpec(memory_space=pltpu.VMEM)] * 4,
        out_specs=pl.BlockSpec(memory_space=pltpu.HBM),
        scratch_shapes=[flat, dma],
        compiler_params=pltpu.CompilerParams(vmem_limit_bytes=16 * 1024 * 1024),
    )(*parts)
    return out.reshape(ND, rows, cols)


def solution(mesh, depth=8):
    grid_rows, grid_cols = mesh.shape["row"], mesh.shape["col"]

    def body(phase, pairs):
        return on_device(grid_rows, grid_cols, depth, phase, pairs)

    return jax.shard_map(
        body,
        mesh=mesh,
        in_specs=(P(None, "row", "col"), P()),
        out_specs=P(None, "row", "col"),
        check_vma=False,
    )
```

```python
import jax
import jax.numpy as jnp
from jax import lax
from jax.experimental import pallas as pl
from jax.experimental.pallas import tpu as pltpu
from jax.sharding import PartitionSpec as P

ND = 128
LAM2 = 0.8 * 0.8
HALO = 5
NEAR = 3
PAD = 16
DIST_COL = 8
MESH = pl.DeviceIdType.MESH
F32 = jnp.float32
BF16 = jnp.bfloat16


def split(x, terms):
    parts = []
    for _ in range(terms - 1):
        parts.append(x.astype(BF16))
        x = x - parts[-1].astype(F32)
    return parts + [x.astype(BF16)]


def krylov_kernel(
    grid_rows, grid_cols, depth_rows,
    phase_ref, pairs_hbm, zt, p1t, p2t, weights,
    pairs_ref, ph, z, w1, q1, w2, q2, nmat, acc, tot, in1, in2,
    pairs_sem, load_sem, halo_send, halo_recv, s1s, s1r, s2s, s2r,
):
    rows, cols = ph.shape[0], ph.shape[2]
    row, col = lax.axis_index("row"), lax.axis_index("col")
    y_len = grid_rows // depth_rows
    row_y, row_z = row // depth_rows, lax.rem(row, depth_rows)

    first, last = PAD, PAD + cols
    total_rows = rows + 2 * HALO

    def clear_sides(e, carry):
        z[e, first - DIST_COL:first, :] = jnp.zeros((DIST_COL, ND), F32)
        z[e, last:last + DIST_COL, :] = jnp.zeros((DIST_COL, ND), F32)
        return carry

    def clear_ends(e, carry):
        for base in (0, HALO + rows):
            z[base + e, first:last, :] = jnp.zeros((cols, ND), F32)
        return carry

    def load(i, r):
        return pltpu.make_async_copy(phase_ref.at[:, r, 0, :], ph.at[r], load_sem.at[i])

    def loaded(i):
        here = ph.at[pl.ds(parts[i].start, len(parts[i]))]
        pltpu.make_async_copy(here, here, load_sem.at[i]).wait()

    top_rows, low_rows = range(0, HALO), range(rows - HALO, rows)
    parts = [top_rows, low_rows, range(HALO, rows // 2), range(rows // 2, rows - HALO)]
    load_pairs = pltpu.make_async_copy(pairs_hbm, pairs_ref, pairs_sem)
    load_pairs.start()
    for r in top_rows:
        load(0, r).start()

    around = [(-1, 0), (1, 0), (0, -1), (0, 1), (-1, -1), (-1, 1), (1, -1), (1, 1)]

    def exists(dr, dc):
        ok = jnp.bool_(True)
        if dr < 0:
            ok = row > 0
        if dr > 0:
            ok = row < grid_rows - 1
        if dc < 0:
            ok = ok & (col > 0)
        if dc > 0:
            ok = ok & (col < grid_cols - 1)
        return ok

    def plane_peer(k):
        other_y = lax.rem(row_y + k // grid_cols, y_len)
        return (other_y * depth_rows + row_z, lax.rem(col + k % grid_cols, grid_cols))

    def z_peer(k):
        return (row_y * depth_rows + lax.rem(row_z + k, depth_rows), col)

    groups = [
        (y_len * grid_cols, plane_peer, in1, s1s, s1r),
        (depth_rows, z_peer, in2, s2s, s2r),
    ]
    barrier = pltpu.get_barrier_semaphore()
    for size, peer, _buf, _s, _r in reversed(groups):
        for k in range(1, size):
            pl.semaphore_signal(barrier, inc=1, device_id=peer(k), device_id_type=MESH)
    for i in (1, 2, 3):
        for r in parts[i]:
            load(i, r).start()
    lax.fori_loop(0, total_rows, clear_sides, 0)
    lax.fori_loop(0, HALO, clear_ends, 0)
    for dr, dc in around:
        @pl.when(exists(dr, dc))
        def _():
            pl.semaphore_signal(barrier, inc=1, device_id=(row + dr, col + dc), device_id_type=MESH)

    load_pairs.wait()
    dates = lax.broadcasted_iota(jnp.int32, (ND, pairs_ref.shape[1]), 0)
    later = (dates == pairs_ref[1:2, :]).astype(F32)
    earlier = (dates == pairs_ref[0:1, :]).astype(F32)
    gt = (later - earlier).astype(BF16)
    normal = lax.dot_general(gt, gt, (((1,), (1,)), ((), ())), preferred_element_type=F32)
    eye = (
        lax.broadcasted_iota(jnp.int32, (ND, ND), 0) == lax.broadcasted_iota(jnp.int32, (ND, ND), 1)
    )
    trace = jnp.sum(jnp.where(eye, normal, 0.0), keepdims=True)
    frob = jnp.sum(normal * normal, keepdims=True)
    shift = jnp.floor(frob / trace + 20.0 * LAM2 + 0.5)
    shifted = normal - jnp.where(eye, shift, 0.0)
    n_hi = shifted.astype(BF16)
    n_lo = (shifted - n_hi.astype(F32)).astype(BF16)
    nmat[...] = jnp.concatenate([n_hi, n_hi, n_hi, n_lo], axis=0)

    left_ok = jnp.where(col > 0, 1.0, 0.0)
    right_ok = jnp.where(col < grid_cols - 1, 1.0, 0.0)
    top_ok = jnp.where(row > 0, 1.0, 0.0)
    bottom_ok = jnp.where(row < grid_rows - 1, 1.0, 0.0)
    def make_z(i, group):
        part = list(parts[i])
        loaded(i)
        for some in [part[at:at + group] for at in range(0, len(part), group)]:
            terms = [split(ph[r], 2) for r in some]
            field = sum(
                jnp.dot(gt, jnp.concatenate([x[t] for x in terms], axis=1), preferred_element_type=F32)
                for t in range(2)
            )
            for j, r in enumerate(some):
                one = field[:, j * cols:(j + 1) * cols]
                zt[r] = one
                z[HALO + r, first:last, :] = one.T

    far = HALO - NEAR
    top, low, end = HALO, rows + HALO, HALO + rows
    half = rows // 2
    pieces = []
    for dr, source, target in ((-1, top, end), (1, low - NEAR, HALO - NEAR)):
        pieces.append((dr, 0, source, target, NEAR))
        source, target = (top, end) if dr < 0 else (low - HALO + 1, 1)
        pieces += [(dr, dc, source, target, HALO - 1) for dc in (-1, 1)]
        source, target = (top + NEAR, end + NEAR) if dr < 0 else (low - HALO, 0)
        pieces.append((dr, 0, source, target, far))
    for r in (0, half):
        pieces += [(0, dc, HALO + r, HALO + r, half) for dc in (-1, 1)]
    near_pieces, far_pieces, side_pieces = (0, 1, 2, 4, 5, 6), (3, 7), (8, 9, 10, 11)

    def halo(i):
        dr, dc, source, target, count = pieces[i]
        width = cols if dc == 0 else HALO - 1 if dr else HALO
        source_col = last - width if dc == 1 else first
        target_col = {-1: last, 0: first, 1: first - width}[dc]
        return pltpu.make_async_remote_copy(
            src_ref=z.at[pl.ds(source, count), pl.ds(source_col, width), :],
            dst_ref=z.at[pl.ds(target, count), pl.ds(target_col, width), :],
            send_sem=halo_send.at[i],
            recv_sem=halo_recv.at[i],
            device_id=(row + dr, col + dc),
            device_id_type=MESH,
        )

    def send(i):
        @pl.when(exists(*pieces[i][:2]))
        def _():
            halo(i).start()

    def arrived(i):
        dr, dc = pieces[i][:2]
        @pl.when(exists(-dr, -dc))
        def _():
            halo(i).wait_recv()

    def sent(i):
        @pl.when(exists(*pieces[i][:2]))
        def _():
            halo(i).wait_send()

    make_z(0, 5)
    make_z(1, 5)
    n_peers = sum(size - 1 for size, *_ in groups)
    n_around = jnp.int32(0)
    for dr, dc in around:
        n_around = n_around + jnp.where(exists(dr, dc), 1, 0)
    pl.semaphore_wait(barrier, n_around + n_peers)
    for i in (0, 4, 1, 2, 5, 6, 3, 7):
        send(i)
    for part, side in ((2, side_pieces[:2]), (3, side_pieces[2:])):
        make_z(part, 4)
        for i in side:
            send(i)

    acc[...] = jnp.zeros_like(acc)

    everything = [(first - DIST_COL, cols + 2 * DIST_COL)]
    own_columns = [(first, cols)]
    inner = [[(first + edge, cols - 2 * edge)] for edge in (8, 16, 24, 32)]
    outer = [[(first - DIST_COL, DIST_COL + edge), (last - edge, DIST_COL + edge)] for edge in (8, 16, 24, 32)]

    def lap(buf, e, span):
        at, width = span
        here = pl.ds(at, width)
        beside = buf[e - 1, here, :] + buf[e + 1, here, :] + buf[e, pl.ds(at - 1, width), :] + buf[e, pl.ds(at + 1, width), :]
        return 4.0 * buf[e, here, :] - beside

    def normal_times(values):
        def times(some):
            pieces = []
            for value in some:
                hi, mid, lo = split(value, 3)
                pieces.append(jnp.concatenate([hi, mid, lo, hi], axis=1))
            both = jnp.dot(jnp.concatenate(pieces, axis=0), nmat[...], preferred_element_type=F32)
            products, at = [], 0
            for value in some:
                products.append(both[at:at + value.shape[0], :])
                at += value.shape[0]
            return products

        half = (len(values) + 1) // 2
        return times(values[:half]) + times(values[half:])

    def own(value, span):
        lo = max(first - span[0], 0)
        return value[lo:lo + min(span[0] + span[1], last) - max(span[0], first), :]

    def folded(value):
        return jnp.sum(value.reshape(value.shape[0] // 8, 8, ND), axis=0)

    def masked(value, span, scale):
        lo, hi = first - span[0], last - span[0]
        parts = [own(value, span)]
        if lo > 0:
            parts = [value[:lo] * left_ok] + parts
        if span[1] > hi:
            parts = parts + [value[hi:] * right_ok]
        value = jnp.concatenate(parts, axis=0) if len(parts) > 1 else parts[0]
        return value if scale is None else value * scale

    def blocks(lo, hi, block, body):
        def step(i, carry):
            body([lo + block * i + j for j in range(block)])
            return carry
        lax.fori_loop(0, (hi - lo) // block, step, 0)

    def scale_of(e):
        if isinstance(e, int):
            return top_ok if e < HALO else bottom_ok if e >= HALO + rows else None
        return None

    def counts(e):
        return not isinstance(e, int) or HALO <= e < HALO + rows

    def lap_rows(src, dst, spans, es):
        for e in es:
            for span in spans:
                dst[e, pl.ds(*span), :] = masked(lap(src, e, span), span, scale_of(e))

    def k_rows(src, lap_buf, dst, moment, spans, es):
        sums = [jnp.zeros((8, ND), F32)] * 3
        places = [(e, span) for e in es for span in spans]
        products = normal_times([src[e, pl.ds(*span), :] for e, span in places])
        for (e, span), product in zip(places, products):
            value = src[e, pl.ds(*span), :]
            result = masked(product + LAM2 * lap(lap_buf, e, span), span, scale_of(e))
            dst[e, pl.ds(*span), :] = result
            if counts(e):
                mine, new = own(value, span), own(result, span)
                if moment == 1:
                    sums[0] = sums[0] + folded(mine * mine)
                sums[1] = sums[1] + folded(mine * new)
                sums[2] = sums[2] + folded(new * new)
        if moment == 1:
            acc[0] += sums[0]
        acc[moment] += sums[1]
        acc[moment + 1] += sums[2]

    def last_rows(spans, es):
        (span,) = spans
        products = normal_times([q2[e, pl.ds(*span), :] for e in es])
        total = jnp.zeros((8, ND), F32)
        for e, product in zip(es, products):
            value, bent = q2[e, pl.ds(*span), :], lap(q2, e, span)
            p1t[e - HALO] = q1[e, first:last, :].T
            p2t[e - HALO] = value.T
            total = total + folded(value * product + LAM2 * (bent * bent))
        acc[5] += total

    stages = [
        lambda spans, es: lap_rows(z, w1, spans, es),
        lambda spans, es: k_rows(z, w1, q1, 1, spans, es),
        lambda spans, es: lap_rows(q1, w2, spans, es),
        lambda spans, es: k_rows(q1, w2, q2, 3, spans, es),
        last_rows,
    ]
    last_stage = len(stages)
    spans_of = [everything] * (last_stage - 1) + [own_columns]

    def middle(k, spans, block):
        blocks(HALO + k, HALO + rows - k, block, lambda es: stages[k - 1](spans, es))

    for k, block in enumerate((3, 14, 2, 12), 1):
        middle(k, inner[k - 1], block)
    for i in side_pieces:
        arrived(i)
    for k, block in enumerate((6, 28, 2, 24), 1):
        middle(k, outer[k - 1], block)
    middle(5, own_columns, 22)

    def ends(done, ready):
        for k, stage in enumerate(stages, 1):
            above = range(HALO - ready + k, HALO - done + k)
            below = range(HALO + rows + done - k, HALO + rows + ready - k)
            stage(spans_of[k - 1], list(above) + list(below))

    for i in near_pieces:
        arrived(i)
    ends(0, NEAR)
    for i in far_pieces:
        arrived(i)
    ends(NEAR, HALO)

    lines = jnp.concatenate([jnp.sum(acc[j], axis=0, keepdims=True) for j in range(8)], axis=0)
    lines = jnp.broadcast_to(jnp.sum(lines, axis=1, keepdims=True), (8, ND))
    at = lax.broadcasted_iota(jnp.int32, (8, ND), 0) == lax.broadcasted_iota(jnp.int32, (8, ND), 1)
    tot[0] = jnp.sum(jnp.where(at, lines, 0.0), axis=0, keepdims=True)

    def group_copy(stage, k):
        size, peer, buf, s_sem, r_sem = groups[stage]
        return pltpu.make_async_remote_copy(
            src_ref=tot.at[stage],
            dst_ref=buf.at[k],
            send_sem=s_sem,
            recv_sem=r_sem,
            device_id=peer(k),
            device_id_type=MESH,
        )

    def all_copies(stage):
        size, peer, buf, s_sem, r_sem = groups[stage]
        others = buf.at[pl.ds(1, size - 1)]
        return pltpu.make_async_remote_copy(
            src_ref=others, dst_ref=others, send_sem=s_sem, recv_sem=r_sem, device_id=peer(1), device_id_type=MESH
        )

    for stage in range(2):
        size = groups[stage][0]
        for k in range(1, size):
            group_copy(stage, k).start()
        if stage == 0:
            for i in range(len(pieces)):
                sent(i)
        all_copies(stage).wait_send()
        all_copies(stage).wait_recv()
        part = tot[stage]
        for k in range(1, size):
            part = part + groups[stage][2][k]
        tot[stage + 1] = part

    lane = lax.broadcasted_iota(jnp.int32, (1, ND), 1)
    mu = []
    for j in range(6):
        mu.append(jnp.broadcast_to(jnp.sum(jnp.where(lane == j, tot[2], 0.0), axis=1, keepdims=True), (1, ND)))
    s = jnp.broadcast_to(shift, (1, ND))
    h00 = mu[1] + s * mu[0]
    h01 = mu[2] + s * mu[1]
    h02 = mu[3] + s * mu[2]
    h11 = h02
    h12 = mu[4] + s * mu[3]
    h22 = mu[5] + s * mu[4]
    l10, l20 = h01 / h00, h02 / h00
    d1 = h11 - l10 * h01
    e1 = h12 - l20 * h01
    l21 = e1 / d1
    d2 = h22 - l20 * h02 - l21 * e1
    y1 = mu[1] - l10 * mu[0]
    y2 = mu[2] - l20 * mu[0] - l21 * y1
    c2 = y2 / d2
    c1 = y1 / d1 - l21 * c2
    c0 = mu[0] / h00 - l10 * c1 - l20 * c2

    weights[...] = jnp.concatenate([c0, c1, c2] + [jnp.zeros((1, ND), F32)] * 5, axis=0)


def store_kernel(zt, p1t, p2t, weights, out_ref, xt, sem):
    rows = zt.shape[0]
    c0, c1, c2 = weights[0:1, :], weights[1:2, :], weights[2:3, :]

    def copy(r):
        return pltpu.make_async_copy(xt.at[r], out_ref.at[:, r, 0, :], sem)

    def combine(r, carry):
        xt[r] = c0 * zt[r] + c1 * p1t[r] + c2 * p2t[r]
        copy(r).start()
        return carry

    lax.fori_loop(0, rows, combine, 0)
    pltpu.make_async_copy(xt, xt, sem).wait()


def on_device(grid_rows, grid_cols, depth_rows, phase, pairs):
    m, rows, cols = phase.shape
    total_rows, total_cols = rows + 2 * HALO, cols + 2 * PAD
    y_len = grid_rows // depth_rows
    field = pltpu.VMEM((total_rows, total_cols, ND), F32)
    flat = pltpu.VMEM((rows, ND, cols), F32)
    dma = pltpu.SemaphoreType.DMA
    pieces = 12
    parts = pl.pallas_call(
        lambda *refs: krylov_kernel(grid_rows, grid_cols, depth_rows, *refs),
        name="krylov",
        out_shape=[jax.ShapeDtypeStruct((rows, ND, cols), F32)] * 3 + [jax.ShapeDtypeStruct((8, ND), F32)],
        in_specs=[pl.BlockSpec(memory_space=pltpu.HBM)] * 2,
        out_specs=[pl.BlockSpec(memory_space=pltpu.VMEM)] * 4,
        scratch_shapes=[
            pltpu.VMEM((2, m), jnp.int32),
            pltpu.VMEM((rows, m, cols), F32),
            field, field, field, field, field,
            pltpu.VMEM((4 * ND, ND), BF16),
            pltpu.VMEM((8, 8, ND), F32),
            pltpu.VMEM((3, 1, ND), F32),
            pltpu.VMEM((y_len * grid_cols, 1, ND), F32),
            pltpu.VMEM((depth_rows, 1, ND), F32),
            dma, dma((4,)),
            dma((pieces,)), dma((pieces,)),
            dma, dma, dma, dma,
        ],
        compiler_params=pltpu.CompilerParams(
            collective_id=0, has_side_effects=True, vmem_limit_bytes=40 * 1024 * 1024
        ),
    )(phase.reshape(m, rows, 1, cols), pltpu.with_memory_space_constraint(pairs.T, pltpu.HBM))
    out = pl.pallas_call(
        store_kernel,
        name="store",
        out_shape=jax.ShapeDtypeStruct((ND, rows, 1, cols), F32),
        in_specs=[pl.BlockSpec(memory_space=pltpu.VMEM)] * 4,
        out_specs=pl.BlockSpec(memory_space=pltpu.HBM),
        scratch_shapes=[flat, dma],
        compiler_params=pltpu.CompilerParams(vmem_limit_bytes=16 * 1024 * 1024),
    )(*parts)
    return out.reshape(ND, rows, cols)


def solution(mesh, depth=8):
    grid_rows, grid_cols = mesh.shape["row"], mesh.shape["col"]

    def body(phase, pairs):
        return on_device(grid_rows, grid_cols, depth, phase, pairs)

    return jax.shard_map(
        body,
        mesh=mesh,
        in_specs=(P(None, "row", "col"), P()),
        out_specs=P(None, "row", "col"),
        check_vma=False,
    )
```
